32 devices in a mesh: dp: 1 (over z), etp: 4 (over y), ep: 8 (over x, core).
Axes of the slice: x: 4, y: 4, z: 1, core: 2. Of those that a mesh axis runs over, the one named last changes fastest.
The devices are a block of a 4x4x8 slice.
Arguments:
- u_rows: bfloat16 [2048, 1536], P(('dp', 'ep', 'etp'))
- dy_rows: bfloat16 [2048, 1536], P(('dp', 'ep', 'etp'))
- topk_ids: int32 [2048, 4], P(('dp', 'ep', 'etp'))
- w_router: bfloat16 [1536, 32], replicated
- w_gate: bfloat16 [32, 1536, 768], P('ep', None, 'etp')
- w_up: bfloat16 [32, 1536, 768], P('ep', None, 'etp')
- w_down: bfloat16 [32, 768, 1536], P('ep', 'etp')
Outputs:
- output 1: bfloat16 [2048, 1536], P(('dp', 'ep', 'etp'))
- output 2: bfloat16 [2048, 1536], P(('dp', 'ep', 'etp'))
- output 3: float32 [32, 1536, 768], P(('dp', 'ep'), None, 'etp')
- output 4: float32 [32, 1536, 768], P(('dp', 'ep'), None, 'etp')
- output 5: float32 [32, 768, 1536], P(('dp', 'ep'), 'etp')
- output 6: float32 [1536, 32], P('dp')
All inputs are finite; a program needn't handle non-finite values.
Results may differ from the reference program's by a relative error of at most 0.0112773.
Values are sent between devices in bfloat16 or wider.
A program may use at most 768 MiB of HBM per device.

```python
import jax
import jax.numpy as jnp
from jax import lax

TOK_DEV = 64
SHARDS = 32
D_MODEL = 1536
EXPERTS = 32
TOP_K = 4
FFN = 768
TOKENS = TOK_DEV * SHARDS
CAP = min(TOK_DEV, (4 * TOK_DEV * TOP_K + EXPERTS - 1) // EXPERTS)
EXP_ROWS = SHARDS * CAP


def shard_ids(shard_key):
    key_perm, key_rank = jax.random.split(shard_key)
    expert_perm = jax.random.permutation(key_perm, EXPERTS)
    tok_rank = jax.random.permutation(key_rank, TOK_DEV)
    hot_expert = expert_perm[EXPERTS - 1]
    slot_col = jnp.arange(TOP_K)[None, :]
    has_hot = (tok_rank < CAP)[:, None]
    base_pos = tok_rank * TOP_K - jnp.minimum(tok_rank, CAP)
    cyc_pos = (base_pos[:, None] + slot_col - has_hot.astype(jnp.int32)) % (EXPERTS - 1)
    chosen = jnp.where(has_hot & (slot_col == 0), hot_expert, expert_perm[cyc_pos])
    return chosen.astype(jnp.int32)


def setup_inputs(seed: int = 0, part: int = 0) -> dict:
    part_key = jax.random.fold_in(jax.random.key(seed), part)
    key_tok, key_cot, key_route = jax.random.split(part_key, 3)
    key_router, key_gate, key_up, key_down = jax.random.split(jax.random.key(seed + 1), 4)
    topk_ids = jax.vmap(shard_ids)(jax.random.split(key_route, SHARDS)).reshape(TOKENS, TOP_K)
    u_rows = jax.random.normal(key_tok, (TOKENS, D_MODEL), jnp.float32).astype(jnp.bfloat16)
    dy_rows = jax.random.normal(key_cot, (TOKENS, D_MODEL), jnp.float32).astype(jnp.bfloat16)
    w_router = (jax.random.normal(key_router, (D_MODEL, EXPERTS), jnp.float32) * D_MODEL ** -0.5).astype(jnp.bfloat16)
    w_gate = (jax.random.normal(key_gate, (EXPERTS, D_MODEL, FFN), jnp.float32) * D_MODEL ** -0.5).astype(jnp.bfloat16)
    w_up = (jax.random.normal(key_up, (EXPERTS, D_MODEL, FFN), jnp.float32) * D_MODEL ** -0.5).astype(jnp.bfloat16)
    down_scale = 4.0 * EXPERTS / TOP_K * FFN ** -0.5
    w_down = (jax.random.normal(key_down, (EXPERTS, FFN, D_MODEL), jnp.float32) * down_scale).astype(jnp.bfloat16)
    return {"u_rows": u_rows, "dy_rows": dy_rows, "topk_ids": topk_ids, "w_router": w_router, "w_gate": w_gate, "w_up": w_up, "w_down": w_down}


def one_expert(u_wide, tok_rows, gate_rows, gate_e, up_e, down_e):
    x_rows = u_wide[tok_rows]
    h_gate = jnp.dot(x_rows, gate_e, preferred_element_type=jnp.float32).astype(jnp.bfloat16).astype(jnp.float32)
    h_up = jnp.dot(x_rows, up_e, preferred_element_type=jnp.float32).astype(jnp.bfloat16).astype(jnp.float32)
    act_rows = (jax.nn.silu(h_gate) * h_up).astype(jnp.bfloat16).astype(jnp.float32)
    out_rows = jnp.dot(act_rows, down_e, preferred_element_type=jnp.float32).astype(jnp.bfloat16).astype(jnp.float32)
    return gate_rows[:, None] * out_rows


def moe_forward(u_wide, topk_ids, router_wide, gate_wide, up_wide, down_wide):
    logits = jnp.dot(u_wide, router_wide, preferred_element_type=jnp.float32)
    router_prob = jax.nn.softmax(logits, axis=-1)
    gate_vals = jnp.take_along_axis(router_prob, topk_ids, axis=1).reshape(-1)
    flat_ids = topk_ids.reshape(-1)
    pair_order = jnp.argsort(flat_ids, stable=True)
    counts = jnp.bincount(flat_ids, length=EXPERTS)
    starts = jnp.cumsum(counts) - counts
    row_pos = jnp.arange(EXP_ROWS)
    is_valid = row_pos[None, :] < counts[:, None]
    pair_idx = pair_order[jnp.minimum(starts[:, None] + row_pos[None, :], TOKENS * TOP_K - 1)]
    tok_idx = pair_idx // TOP_K
    row_gate = jnp.where(is_valid, gate_vals[pair_idx], 0.0)
    expert_fn = jax.checkpoint(one_expert)

    def expert_step(moe_sum, per_expert):
        tok_rows, gate_rows, gate_e, up_e, down_e = per_expert
        contrib = expert_fn(u_wide, tok_rows, gate_rows, gate_e, up_e, down_e)
        return moe_sum.at[tok_rows].add(contrib), None

    moe_sum, unused = lax.scan(expert_step, jnp.zeros((TOKENS, D_MODEL), jnp.float32), (tok_idx, row_gate, gate_wide, up_wide, down_wide))
    return (u_wide + moe_sum).astype(jnp.bfloat16)


def reference(u_rows, dy_rows, topk_ids, w_router, w_gate, w_up, w_down):
    def forward(u_wide, router_wide, gate_wide, up_wide, down_wide):
        return moe_forward(u_wide, topk_ids, router_wide, gate_wide, up_wide, down_wide)

    y_rows, pull_back = jax.vjp(forward, u_rows.astype(jnp.float32), w_router.astype(jnp.float32), w_gate.astype(jnp.float32), w_up.astype(jnp.float32), w_down.astype(jnp.float32))
    du_wide, dw_router, dw_gate, dw_up, dw_down = pull_back(dy_rows)
    return y_rows, du_wide.astype(jnp.bfloat16), dw_gate, dw_up, dw_down, dw_router
```

```python
import jax
import jax.numpy as jnp
from jax import lax
from jax.sharding import PartitionSpec as P


def dot_f32(lhs, rhs, contract):
    return lax.dot_general(lhs, rhs, (contract, ((), ())), preferred_element_type=jnp.float32)


def solution(mesh):
    tok_spec = P(("dp", "ep", "etp"), None)
    col_spec = P("ep", None, "etp")
    row_spec = P("ep", "etp", None)
    in_specs = (tok_spec, tok_spec, tok_spec, P(None, None), col_spec, col_spec, row_spec)
    out_specs = (tok_spec, tok_spec, P(("dp", "ep"), None, "etp"), P(("dp", "ep"), None, "etp"), P(("dp", "ep"), "etp", None), P("dp", None))
    axes = ("ep", "etp")

    def device_step(u_loc, dy_loc, ids_loc, w_router, w_gate, w_up, w_down):
        experts = w_router.shape[1]
        local_exp, d_model, width = w_gate.shape
        logits = jnp.dot(u_loc, w_router, preferred_element_type=jnp.float32)
        prob = jax.nn.softmax(logits, axis=-1)
        hot = jnp.any(ids_loc[:, :, None] == jnp.arange(experts, dtype=jnp.int32)[None, None, :], axis=1)
        gate_loc = jnp.where(hot, prob, 0.0)
        u_all = lax.all_gather(u_loc, axes, axis=0, tiled=True)
        dy_all = lax.all_gather(dy_loc, axes, axis=0, tiled=True)
        gate_all = lax.all_gather(gate_loc, axes, axis=0, tiled=True)
        first = lax.axis_index("ep") * local_exp
        gate = lax.dynamic_slice_in_dim(gate_all, first, local_exp, axis=1)
        gate_wide = jnp.repeat(gate, width, axis=1)
        w1 = jnp.swapaxes(w_gate, 1, 2).reshape(local_exp * width, d_model)
        w3 = jnp.swapaxes(w_up, 1, 2).reshape(local_exp * width, d_model)
        w2 = w_down.reshape(local_exp * width, d_model)
        nt = ((1,), (1,))
        nn = ((1,), (0,))
        tn = ((0,), (0,))
        h1 = dot_f32(u_all, w1, nt).astype(jnp.bfloat16).astype(jnp.float32)
        h3 = dot_f32(u_all, w3, nt).astype(jnp.bfloat16).astype(jnp.float32)
        q = dot_f32(dy_all, w2, nt)
        live = gate_wide > 0
        sig = jax.nn.sigmoid(h1)
        silu = h1 * sig
        act = (silu * h3).astype(jnp.bfloat16).astype(jnp.float32)
        act = jnp.where(live, act, 0.0)
        ga = (gate_wide * act).astype(jnp.bfloat16)
        da = jnp.where(live, gate_wide * q, 0.0).astype(jnp.bfloat16).astype(jnp.float32)
        dgate = jnp.sum((act * q).reshape(-1, local_exp, width), axis=2)
        dh1 = jnp.where(live, da * h3 * sig * (1.0 + h1 * (1.0 - sig)), 0.0).astype(jnp.bfloat16)
        dh3 = jnp.where(live, da * silu, 0.0).astype(jnp.bfloat16)
        y_part = dot_f32(ga, w2, nn)
        du_part = dot_f32(dh1, w1, nn) + dot_f32(dh3, w3, nn)
        dw1 = dot_f32(dh1, u_all, tn)
        dw3 = dot_f32(dh3, u_all, tn)
        dw2 = dot_f32(ga, dy_all, tn)
        y_own = lax.psum_scatter(y_part, axes, scatter_dimension=0, tiled=True)
        du_own = lax.psum_scatter(du_part, axes, scatter_dimension=0, tiled=True)
        dg_wide = lax.dynamic_update_slice_in_dim(jnp.zeros_like(gate_all), dgate, first, axis=1)
        dg_loc = lax.psum_scatter(dg_wide, axes, scatter_dimension=0, tiled=True)
        d_logit = prob * (dg_loc - jnp.sum(prob * dg_loc, axis=-1, keepdims=True))
        dw_router = lax.psum(dot_f32(u_loc, d_logit.astype(jnp.bfloat16), tn), axes)
        du_router = dot_f32(d_logit.astype(jnp.bfloat16), w_router, nt)
        y_loc = (u_loc.astype(jnp.float32) + y_own).astype(jnp.bfloat16)
        du_loc = (dy_loc.astype(jnp.float32) + du_own + du_router).astype(jnp.bfloat16)
        unfold = lambda d: jnp.swapaxes(d.reshape(local_exp, width, d_model), 1, 2)
        return y_loc, du_loc, unfold(dw1), unfold(dw3), dw2.reshape(local_exp, width, d_model), dw_router

    return jax.shard_map(device_step, mesh=mesh, in_specs=in_specs, out_specs=out_specs, check_vma=False)
```

```python
import functools

import jax
import jax.numpy as jnp
from jax import lax
from jax.experimental import pallas as pl
from jax.experimental.pallas import tpu as pltpu
from jax.sharding import PartitionSpec as P

MESH = pl.DeviceIdType.MESH
RELS = (2, 1, 3, 0)


def wait_all(copies):
    for copy in copies:
        copy.wait_send()


def reduce_kernel(etp_size, y_hbm, du_hbm, u_hbm, dg_ref, u_ref, dy_ref, wr_ref, prob_ref, y_out, du_out, dwr_out,
                  mine, peer, relay, inbox, total, stage, relay2, inbox2, u_all, dg_in, dl_in, dl_out,
                  load_sem, send_sem, recv_sem, dg_send, dg_recv, dl_send, dl_recv):
    ep_size = mine.shape[1] * 2
    ring = mine.shape[1]
    count = ep_size * etp_size
    ep, etp = lax.axis_index("ep"), lax.axis_index("etp")
    col, core = ep // 2, ep % 2
    lin = ep * etp_size + etp
    tok = u_ref.shape[0]
    half = tok // 2
    local_exp = wr_ref.shape[0] // ep_size
    spots = ((col, etp), (etp, col))

    def at_x(step):
        return {"ep": lax.rem(col + step + ring, ring) * 2 + core, "etp": etp}

    def at_y(step):
        return {"ep": ep, "etp": lax.rem(etp + step + etp_size, etp_size)}

    first_axis = (at_x, at_y)
    second_axis = (at_y, at_x)
    source = (y_hbm, du_hbm)

    loads = []
    for rel in RELS:
        for arr in range(2):
            pos = lax.rem(spots[arr][0] + rel, ring)
            src = y_hbm.at[pos, core] if arr == 0 else du_hbm.at[:, core, pos]
            copy = pltpu.make_async_copy(src, mine.at[arr, pos], load_sem.at[arr, rel])
            copy.start()
            loads.append(copy)
    u_load = pltpu.make_async_copy(u_hbm, u_all, load_sem.at[2, 0])
    u_load.start()

    barrier = pltpu.get_barrier_semaphore()

    def other(step):
        dest = lax.rem(lin + step, count)
        return {"ep": dest // etp_size, "etp": lax.rem(dest, etp_size)}, dest

    def greet(step, carry):
        pl.semaphore_signal(barrier, inc=1, device_id=other(step)[0], device_id_type=MESH)
        return carry

    lax.fori_loop(1, count, greet, 0)
    pl.semaphore_wait(barrier, count - 1)

    def dg_copy(step):
        device, dest = other(step)
        return pltpu.make_async_remote_copy(dg_ref.at[dest], dg_in.at[lin], dg_send.at[step], dg_recv.at[lin], device_id=device, device_id_type=MESH)

    def dl_copy(step):
        device, dest = other(step)
        return pltpu.make_async_remote_copy(dl_out, dl_in.at[lin], dl_send.at[step], dl_recv.at[lin], device_id=device, device_id_type=MESH)

    def start_dg(step, carry):
        dg_copy(step).start()
        return carry

    lax.fori_loop(1, count, start_dg, 0)
    dg_in[lin] = dg_ref[lin]

    sends = []
    slots = [0]

    def send(src, dst, device):
        slot = slots[0]
        slots[0] += 1
        copy = pltpu.make_async_remote_copy(src, dst, send_sem.at[slot], recv_sem.at[slot], device_id=device, device_id_type=MESH)
        copy.start()
        sends.append(copy)
        return copy

    partner = {"ep": col * 2 + 1 - core, "etp": etp}
    swaps = {}
    for rel in RELS:
        for arr in range(2):
            pos = lax.rem(spots[arr][0] + rel, ring)
            src = y_hbm.at[pos, 1 - core] if arr == 0 else du_hbm.at[:, 1 - core, pos]
            swaps[arr, rel] = send(src, peer.at[arr, pos], partner)

    def ready(arr, rel):
        loads[RELS.index(rel) * 2 + arr].wait()
        swaps[arr, rel].wait_recv()

    def place(arr, rel):
        return lax.rem(spots[arr][0] + rel, ring)

    def inner(arr, sub):
        return lax.rem(spots[arr][1] + sub, ring)

    def value(arr, rel, sub):
        pos, idx = place(arr, rel), inner(arr, sub)
        return mine[arr, pos, idx].astype(jnp.float32) + peer[arr, pos, idx].astype(jnp.float32)

    def put(arr, rel, sub, val):
        mine[arr, place(arr, rel), inner(arr, sub)] = val.astype(jnp.bfloat16)
        return mine.at[arr, place(arr, rel), inner(arr, sub)]

    hops = {}
    for arr in range(2):
        ready(arr, 2)
        for slot, sub, step in ((0, 2, 1), (2, 3, -1), (1, 1, 1), (3, 0, -1)):
            hops["far", arr, sub] = send(put(arr, 2, sub, value(arr, 2, sub)), relay.at[arr, slot], first_axis[arr](step))
    for arr in range(2):
        ready(arr, 1)
        ready(arr, 3)
        for sub_r, sub_l in ((3, 2), (0, 1)):
            hops["left", arr, sub_r] = send(put(arr, 1, sub_r, value(arr, 1, sub_r)), inbox.at[arr, 0, sub_r], first_axis[arr](1))
            hops["right", arr, sub_l] = send(put(arr, 3, sub_l, value(arr, 3, sub_l)), inbox.at[arr, 1, sub_l], first_axis[arr](-1))

    def wait_dg(step, carry):
        src = lax.rem(lin + step, count)
        pltpu.make_async_copy(dg_ref.at[0], dg_in.at[src], dg_recv.at[src]).wait()
        return carry

    lax.fori_loop(1, count, wait_dg, 0)
    rows = []
    for group in range(ep_size):
        tile = dg_in[group * etp_size]
        for part in range(1, etp_size):
            tile = tile + dg_in[group * etp_size + part]
        rows.append(tile[:local_exp])
    d_gate = jnp.concatenate(rows, axis=0)
    prob = prob_ref[...]
    d_logit = prob * (d_gate - jnp.sum(prob * d_gate, axis=0, keepdims=True))
    dl_out[...] = d_logit.astype(jnp.bfloat16)
    dl_in[lin] = d_logit.astype(jnp.bfloat16)

    def start_dl(step, carry):
        dl_copy(step).start()
        return carry

    lax.fori_loop(1, count, start_dl, 0)

    for slot_r, sub_r, slot_l, sub_l in ((0, 2, 2, 3), (1, 1, 3, 0)):
        for arr in range(2):
            hops["far", arr, sub_r].wait_recv()
            val = value(arr, 1, sub_r) + relay[arr, slot_r].astype(jnp.float32)
            hops["left", arr, sub_r] = send(put(arr, 1, sub_r, val), inbox.at[arr, 0, sub_r], first_axis[arr](1))
            hops["far", arr, sub_l].wait_recv()
            val = value(arr, 3, sub_l) + relay[arr, slot_l].astype(jnp.float32)
            hops["right", arr, sub_l] = send(put(arr, 3, sub_l, val), inbox.at[arr, 1, sub_l], first_axis[arr](-1))

    for arr in range(2):
        ready(arr, 0)

    def settle(arr, sub):
        hops["left", arr, sub].wait_recv()
        hops["right", arr, sub].wait_recv()
        return value(arr, 0, sub) + inbox[arr, 0, sub].astype(jnp.float32) + inbox[arr, 1, sub].astype(jnp.float32)

    def ship(arr, sub, part, val, dst, step):
        rows_at = pl.ds(part * half, half)
        stage[arr, sub - 1, rows_at] = val.astype(jnp.bfloat16)
        return send(stage.at[arr, sub - 1, rows_at], dst, second_axis[arr](step))

    for arr in range(2):
        val = settle(arr, 2)
        hops["far2", arr, 0] = ship(arr, 2, 0, val[:half], relay2.at[arr, 0], 1)
        hops["far2", arr, 1] = ship(arr, 2, 1, val[half:], relay2.at[arr, 1], -1)
    for arr in range(2):
        val = settle(arr, 1)
        hops["left2", arr, 1] = ship(arr, 1, 1, val[half:], inbox2.at[arr, 0, 1], 1)
        total[arr, 0, :half] = val[:half]
        val = settle(arr, 3)
        hops["right2", arr, 0] = ship(arr, 3, 0, val[:half], inbox2.at[arr, 1, 0], -1)
        total[arr, 0, half:] = val[half:]
    for arr in range(2):
        hops["far2", arr, 0].wait_recv()
        val = total[arr, 0, :half] + relay2[arr, 0].astype(jnp.float32)
        hops["left2", arr, 0] = ship(arr, 1, 0, val, inbox2.at[arr, 0, 0], 1)
        hops["far2", arr, 1].wait_recv()
        val = total[arr, 0, half:] + relay2[arr, 1].astype(jnp.float32)
        hops["right2", arr, 1] = ship(arr, 3, 1, val, inbox2.at[arr, 1, 1], -1)
    for arr in range(2):
        total[arr, 1] = settle(arr, 0)

    def wait_dl(step, carry):
        src = lax.rem(lin + step, count)
        pltpu.make_async_copy(dl_out, dl_in.at[src], dl_recv.at[src]).wait()
        return carry

    lax.fori_loop(1, count, wait_dl, 0)
    u_load.wait()
    du_router = lax.dot_general(dl_out[...], wr_ref[...], (((0,), (0,)), ((), ())), preferred_element_type=jnp.float32)[:tok]
    span = 8
    dwr_out[...] = jnp.zeros_like(dwr_out)

    def dwr_step(idx, carry):
        parts = []
        for pair in range(span // 2):
            low = dl_in[idx * span + 2 * pair].astype(jnp.float32)
            high = dl_in[idx * span + 2 * pair + 1].astype(jnp.float32)
            parts.append((low + pltpu.roll(high, tok, 1)).astype(jnp.bfloat16))
        lhs = jnp.concatenate(parts, axis=1)
        rhs = u_all[pl.ds(pl.multiple_of(idx * span * tok, span * tok), span * tok)]
        dwr_out[...] += jnp.dot(lhs, rhs, preferred_element_type=jnp.float32)
        return carry

    lax.fori_loop(0, count // span, dwr_step, 0)

    for arr, base, out in ((0, u_ref, y_out), (1, dy_ref, du_out)):
        for part in range(2):
            hops["left2", arr, part].wait_recv()
            hops["right2", arr, part].wait_recv()
            rows_at = pl.ds(part * half, half)
            val = base[rows_at].astype(jnp.float32) + total[arr, 1, rows_at] + inbox2[arr, 0, part].astype(jnp.float32) + inbox2[arr, 1, part].astype(jnp.float32)
            if arr == 1:
                val = val + du_router[part * half:(part + 1) * half]
            out[rows_at] = val.astype(jnp.bfloat16)
    wait_all(sends)

    def drain(step, carry):
        dg_copy(step).wait_send()
        dl_copy(step).wait_send()
        return carry

    lax.fori_loop(1, count, drain, 0)


def reduce_call(mesh, y_part, du_part, u_all, dg_tiles, u_loc, dy_loc, wr_t, prob_t):
    etp_size, ep_size = mesh.shape["etp"], mesh.shape["ep"]
    tok, d_model = u_loc.shape
    count, ring, half = etp_size * ep_size, ep_size // 2, tok // 2
    assert ring == 4 and etp_size == 4
    shape5 = (ring, 2, etp_size, tok, d_model)
    vmem = pl.BlockSpec(memory_space=pltpu.VMEM)
    hbm = pl.BlockSpec(memory_space=pl.ANY)
    bf16, f32 = jnp.bfloat16, jnp.float32
    dma = pltpu.SemaphoreType.DMA
    return pl.pallas_call(
        functools.partial(reduce_kernel, etp_size),
        out_shape=(jax.ShapeDtypeStruct((tok, d_model), bf16), jax.ShapeDtypeStruct((tok, d_model), bf16), jax.ShapeDtypeStruct(wr_t.shape, f32)),
        in_specs=[hbm, hbm, hbm, vmem, vmem, vmem, vmem, vmem],
        out_specs=(vmem, vmem, vmem),
        scratch_shapes=[
            pltpu.VMEM((2, 4, 4, tok, d_model), bf16),
            pltpu.VMEM((2, 4, 4, tok, d_model), bf16),
            pltpu.VMEM((2, 4, tok, d_model), bf16),
            pltpu.VMEM((2, 2, 4, tok, d_model), bf16),
            pltpu.VMEM((2, 2, tok, d_model), f32),
            pltpu.VMEM((2, 3, tok, d_model), bf16),
            pltpu.VMEM((2, 2, half, d_model), bf16),
            pltpu.VMEM((2, 2, 2, half, d_model), bf16),
            pltpu.VMEM((count * tok, d_model), bf16),
            pltpu.VMEM((count, 8, 128), f32),
            pltpu.VMEM((count, wr_t.shape[0], 128), bf16),
            pltpu.VMEM((wr_t.shape[0], 128), bf16),
            dma((3, 4)), dma((48,)), dma((48,)), dma((count,)), dma((count,)), dma((count,)), dma((count,)),
        ],
        compiler_params=pltpu.CompilerParams(collective_id=1, has_side_effects=True, vmem_limit_bytes=48 * 1024 * 1024),
        name="reduce_back",
    )(y_part.reshape(shape5), du_part.reshape(shape5), u_all, dg_tiles, u_loc, dy_loc, wr_t, prob_t)


def dot_f32(lhs, rhs, contract):
    return lax.dot_general(lhs, rhs, (contract, ((), ())), preferred_element_type=jnp.float32)


def solution(mesh):
    tok_spec = P(("dp", "ep", "etp"), None)
    col_spec = P("ep", None, "etp")
    row_spec = P("ep", "etp", None)
    in_specs = (tok_spec, tok_spec, tok_spec, P(None, None), col_spec, col_spec, row_spec)
    out_specs = (tok_spec, tok_spec, P(("dp", "ep"), None, "etp"), P(("dp", "ep"), None, "etp"), P(("dp", "ep"), "etp", None), P("dp", None))
    axes = ("ep", "etp")

    def device_step(u_loc, dy_loc, ids_loc, w_router, w_gate, w_up, w_down):
        experts = w_router.shape[1]
        local_exp, d_model, width = w_gate.shape
        logits = jnp.dot(u_loc, w_router, preferred_element_type=jnp.float32)
        prob = jax.nn.softmax(logits, axis=-1)
        hot = jnp.any(ids_loc[:, :, None] == jnp.arange(experts, dtype=jnp.int32)[None, None, :], axis=1)
        gate_loc = jnp.where(hot, prob, 0.0)
        u_all = lax.all_gather(u_loc, axes, axis=0, tiled=True)
        dy_all = lax.all_gather(dy_loc, axes, axis=0, tiled=True)
        gate_all = lax.all_gather(gate_loc, axes, axis=0, tiled=True)
        first = lax.axis_index("ep") * local_exp
        gate = lax.dynamic_slice_in_dim(gate_all, first, local_exp, axis=1)
        gate_wide = jnp.repeat(gate, width, axis=1)
        w1 = jnp.swapaxes(w_gate, 1, 2).reshape(local_exp * width, d_model)
        w3 = jnp.swapaxes(w_up, 1, 2).reshape(local_exp * width, d_model)
        w2 = w_down.reshape(local_exp * width, d_model)
        nt = ((1,), (1,))
        nn = ((1,), (0,))
        tn = ((0,), (0,))
        h1 = dot_f32(u_all, w1, nt).astype(jnp.bfloat16).astype(jnp.float32)
        h3 = dot_f32(u_all, w3, nt).astype(jnp.bfloat16).astype(jnp.float32)
        q = dot_f32(dy_all, w2, nt)
        live = gate_wide > 0
        sig = jax.nn.sigmoid(h1)
        silu = h1 * sig
        act = (silu * h3).astype(jnp.bfloat16).astype(jnp.float32)
        act = jnp.where(live, act, 0.0)
        ga = (gate_wide * act).astype(jnp.bfloat16)
        da = jnp.where(live, gate_wide * q, 0.0).astype(jnp.bfloat16).astype(jnp.float32)
        dgate = jnp.sum((act * q).reshape(-1, local_exp, width), axis=2)
        dh1 = jnp.where(live, da * h3 * sig * (1.0 + h1 * (1.0 - sig)), 0.0).astype(jnp.bfloat16)
        dh3 = jnp.where(live, da * silu, 0.0).astype(jnp.bfloat16)
        y_part = dot_f32(ga, w2, nn)
        du_part = dot_f32(dh1, w1, nn) + dot_f32(dh3, w3, nn)
        dw1 = dot_f32(dh1, u_all, tn)
        dw3 = dot_f32(dh3, u_all, tn)
        dw2 = dot_f32(ga, dy_all, tn)
        tok, top_k = ids_loc.shape
        count = u_all.shape[0] // tok
        dg_tiles = jnp.pad(jnp.swapaxes(dgate.reshape(count, tok, local_exp), 1, 2), ((0, 0), (0, 8 - local_exp), (0, 128 - tok)))
        prob_t = jnp.pad(prob.T, ((0, 0), (0, 128 - tok)))
        y_loc, du_loc, dwr_t = reduce_call(mesh, y_part.astype(jnp.bfloat16), du_part.astype(jnp.bfloat16), u_all, dg_tiles, u_loc, dy_loc, w_router.T, prob_t)
        dw_router = dwr_t.T
        unfold = lambda d: jnp.swapaxes(d.reshape(local_exp, width, d_model), 1, 2)
        return y_loc, du_loc, unfold(dw1), unfold(dw3), dw2.reshape(local_exp, width, d_model), dw_router

    return jax.shard_map(device_step, mesh=mesh, in_specs=in_specs, out_specs=out_specs, check_vma=False)
```

```python
import functools

import jax
import jax.numpy as jnp
from jax import lax
from jax.experimental import pallas as pl
from jax.experimental.pallas import tpu as pltpu
from jax.sharding import PartitionSpec as P

MESH = pl.DeviceIdType.MESH
PAIR = range(2)


def each_other(count, step):
    lax.fori_loop(1, count, step, 0)


RELS = (2, 1, 3, 0)


def wait_all(copies):
    for copy in copies:
        copy.wait_send()


def reduce_kernel(etp_size, y_hbm, du_hbm, all_hbm, act_hbm, dg_ref, u_ref, dy_ref, wr_ref, prob_ref, y_out, du_out, dwr_out, dw1_hbm, dw3_hbm, dw2_hbm,
                  mine, peer, relay, inbox, total, stage, relay2, inbox2, all_rows, acts, dw_buf, dg_in, dl_in, dl_out,
                  load_sem, act_sem, dw_sem, send_sem, recv_sem, dg_send, dg_recv, dl_send, dl_recv):
    ep_size = mine.shape[1] * 2
    ring = mine.shape[1]
    count = ep_size * etp_size
    ep, etp = lax.axis_index("ep"), lax.axis_index("etp")
    col, core = ep // 2, ep % 2
    lin = ep * etp_size + etp
    tok = u_ref.shape[0]
    half = tok // 2
    local_exp = wr_ref.shape[0] // ep_size
    spots = ((col, etp), (etp, col))

    def at_x(step):
        return {"ep": lax.rem(col + step + ring, ring) * 2 + core, "etp": etp}

    def at_y(step):
        return {"ep": ep, "etp": lax.rem(etp + step + etp_size, etp_size)}

    first_axis = (at_x, at_y)
    second_axis = (at_y, at_x)
    source = (y_hbm, du_hbm)

    loads = []
    for rel in RELS:
        for arr in PAIR:
            pos = lax.rem(spots[arr][0] + rel, ring)
            src = y_hbm.at[pos, core] if arr == 0 else du_hbm.at[:, core, pos]
            copy = pltpu.make_async_copy(src, mine.at[arr, pos], load_sem.at[arr, rel])
            copy.start()
            loads.append(copy)
    row_loads = [pltpu.make_async_copy(all_hbm.at[arr], all_rows.at[arr], load_sem.at[2, arr]) for arr in PAIR]
    act_loads = [pltpu.make_async_copy(act_hbm.at[kind], acts.at[kind], act_sem.at[kind]) for kind in range(3)]
    for copy in (row_loads[0], act_loads[0], act_loads[1], row_loads[1], act_loads[2]):
        copy.start()

    barrier = pltpu.get_barrier_semaphore()

    def other(step):
        dest = lax.rem(lin + step, count)
        return {"ep": dest // etp_size, "etp": lax.rem(dest, etp_size)}, dest

    def greet(step, carry):
        pl.semaphore_signal(barrier, inc=1, device_id=other(step)[0], device_id_type=MESH)
        return carry

    each_other(count, greet)
    pl.semaphore_wait(barrier, count - 1)

    def dg_copy(step):
        device, dest = other(step)
        return pltpu.make_async_remote_copy(dg_ref.at[dest], dg_in.at[lin], dg_send.at[step], dg_recv.at[lin], device_id=device, device_id_type=MESH)

    def dl_copy(step):
        device, dest = other(step)
        return pltpu.make_async_remote_copy(dl_out, dl_in.at[lin], dl_send.at[step], dl_recv.at[lin], device_id=device, device_id_type=MESH)

    def start_dg(step, carry):
        dg_copy(step).start()
        return carry

    each_other(count, start_dg)
    dg_in[lin] = dg_ref[lin]

    dw_outs = (dw1_hbm, dw3_hbm, dw2_hbm)
    inner, d_model = dw1_hbm.shape
    chunk = 256
    chunks = inner // chunk
    pending = {}

    def dw_step(index):
        kind, part = divmod(index, chunks)
        if part == 0:
            act_loads[kind].wait()
            if kind != 1:
                row_loads[kind // 2].wait()
        slot = index % 2
        if slot in pending:
            pending[slot].wait()
        lhs = acts[kind, :, part * chunk:(part + 1) * chunk]
        dw_buf[slot] = lax.dot_general(lhs, all_rows[kind // 2], (((0,), (0,)), ((), ())), preferred_element_type=jnp.float32)
        pending[slot] = pltpu.make_async_copy(dw_buf.at[slot], dw_outs[kind].at[pl.ds(part * chunk, chunk)], dw_sem.at[slot])
        pending[slot].start()

    sends = []
    slots = [0]

    def send(src, dst, device):
        slot = slots[0]
        slots[0] += 1
        copy = pltpu.make_async_remote_copy(src, dst, send_sem.at[slot], recv_sem.at[slot], device_id=device, device_id_type=MESH)
        copy.start()
        sends.append(copy)
        return copy

    partner = {"ep": col * 2 + 1 - core, "etp": etp}
    swaps = {}
    for rel in RELS:
        for arr in PAIR:
            pos = lax.rem(spots[arr][0] + rel, ring)
            src = y_hbm.at[pos, 1 - core] if arr == 0 else du_hbm.at[:, 1 - core, pos]
            swaps[arr, rel] = send(src, peer.at[arr, pos], partner)

    def ready(arr, rel):
        loads[RELS.index(rel) * 2 + arr].wait()
        swaps[arr, rel].wait_recv()

    def place(arr, rel):
        return lax.rem(spots[arr][0] + rel, ring)

    def inner(arr, sub):
        return lax.rem(spots[arr][1] + sub, ring)

    def value(arr, rel, sub):
        pos, idx = place(arr, rel), inner(arr, sub)
        return mine[arr, pos, idx].astype(jnp.float32) + peer[arr, pos, idx].astype(jnp.float32)

    def put(arr, rel, sub, val):
        mine[arr, place(arr, rel), inner(arr, sub)] = val.astype(jnp.bfloat16)
        return mine.at[arr, place(arr, rel), inner(arr, sub)]

    hops = {}
    for arr in PAIR:
        ready(arr, 2)
        for slot, sub, step in ((0, 2, 1), (2, 3, -1), (1, 1, 1), (3, 0, -1)):
            hops["far", arr, sub] = send(put(arr, 2, sub, value(arr, 2, sub)), relay.at[arr, slot], first_axis[arr](step))
    for arr in PAIR:
        ready(arr, 1)
        ready(arr, 3)
        for sub_r, sub_l in ((3, 2), (0, 1)):
            hops["left", arr, sub_r] = send(put(arr, 1, sub_r, value(arr, 1, sub_r)), inbox.at[arr, 0, sub_r], first_axis[arr](1))
            hops["right", arr, sub_l] = send(put(arr, 3, sub_l, value(arr, 3, sub_l)), inbox.at[arr, 1, sub_l], first_axis[arr](-1))

    for index in range(3):
        dw_step(index)

    def wait_dg(step, carry):
        src = lax.rem(lin + step, count)
        pltpu.make_async_copy(dg_ref.at[0], dg_in.at[src], dg_recv.at[src]).wait()
        return carry

    each_other(count, wait_dg)
    rows = []
    for group in range(ep_size):
        tile = dg_in[group * etp_size]
        for part in range(1, etp_size):
            tile = tile + dg_in[group * etp_size + part]
        rows.append(tile[:local_exp])
    d_gate = jnp.concatenate(rows, axis=0)
    prob = prob_ref[...]
    d_logit = prob * (d_gate - jnp.sum(prob * d_gate, axis=0, keepdims=True))
    dl_out[...] = d_logit.astype(jnp.bfloat16)
    dl_in[lin] = d_logit.astype(jnp.bfloat16)

    def start_dl(step, carry):
        dl_copy(step).start()
        return carry

    each_other(count, start_dl)

    for slot_r, sub_r, slot_l, sub_l in ((0, 2, 2, 3), (1, 1, 3, 0)):
        for index in range(3 + slot_r * 2, 5 + slot_r * 2):
            dw_step(index)
        for arr in PAIR:
            hops["far", arr, sub_r].wait_recv()
            val = value(arr, 1, sub_r) + relay[arr, slot_r].astype(jnp.float32)
            hops["left", arr, sub_r] = send(put(arr, 1, sub_r, val), inbox.at[arr, 0, sub_r], first_axis[arr](1))
            hops["far", arr, sub_l].wait_recv()
            val = value(arr, 3, sub_l) + relay[arr, slot_l].astype(jnp.float32)
            hops["right", arr, sub_l] = send(put(arr, 3, sub_l, val), inbox.at[arr, 1, sub_l], first_axis[arr](-1))

    for arr in PAIR:
        ready(arr, 0)
    for index in range(7, 9):
        dw_step(index)

    def settle(arr, sub):
        hops["left", arr, sub].wait_recv()
        hops["right", arr, sub].wait_recv()
        return value(arr, 0, sub) + inbox[arr, 0, sub].astype(jnp.float32) + inbox[arr, 1, sub].astype(jnp.float32)

    def ship(arr, sub, part, val, dst, step):
        rows_at = pl.ds(part * half, half)
        stage[arr, sub - 1, rows_at] = val.astype(jnp.bfloat16)
        return send(stage.at[arr, sub - 1, rows_at], dst, second_axis[arr](step))

    for arr in PAIR:
        val = settle(arr, 2)
        hops["far2", arr, 0] = ship(arr, 2, 0, val[:half], relay2.at[arr, 0], 1)
        hops["far2", arr, 1] = ship(arr, 2, 1, val[half:], relay2.at[arr, 1], -1)
    for arr in PAIR:
        val = settle(arr, 1)
        hops["left2", arr, 1] = ship(arr, 1, 1, val[half:], inbox2.at[arr, 0, 1], 1)
        total[arr, 0, :half] = val[:half]
        val = settle(arr, 3)
        hops["right2", arr, 0] = ship(arr, 3, 0, val[:half], inbox2.at[arr, 1, 0], -1)
        total[arr, 0, half:] = val[half:]
    for arr in PAIR:
        hops["far2", arr, 0].wait_recv()
        val = total[arr, 0, :half] + relay2[arr, 0].astype(jnp.float32)
        hops["left2", arr, 0] = ship(arr, 1, 0, val, inbox2.at[arr, 0, 0], 1)
        hops["far2", arr, 1].wait_recv()
        val = total[arr, 0, half:] + relay2[arr, 1].astype(jnp.float32)
        hops["right2", arr, 1] = ship(arr, 3, 1, val, inbox2.at[arr, 1, 1], -1)
    for arr in PAIR:
        total[arr, 1] = settle(arr, 0)

    def wait_dl(step, carry):
        src = lax.rem(lin + step, count)
        pltpu.make_async_copy(dl_out, dl_in.at[src], dl_recv.at[src]).wait()
        return carry

    each_other(count, wait_dl)
    du_router = lax.dot_general(dl_out[...], wr_ref[...], (((0,), (0,)), ((), ())), preferred_element_type=jnp.float32)[:tok]
    span = 8
    dwr_out[...] = jnp.zeros_like(dwr_out)

    def dwr_step(idx, carry):
        parts = []
        for pair in range(span // 2):
            low = dl_in[idx * 2 * etp_size + pair].astype(jnp.float32)
            high = dl_in[(idx * 2 + 1) * etp_size + pair].astype(jnp.float32)
            parts.append((low + pltpu.roll(high, tok, 1)).astype(jnp.bfloat16))
        lhs = jnp.concatenate(parts, axis=1)
        rhs = all_rows[0, pl.ds(pl.multiple_of(idx * span * tok, span * tok), span * tok)]
        dwr_out[...] += jnp.dot(lhs, rhs, preferred_element_type=jnp.float32)
        return carry

    lax.fori_loop(0, count // span, dwr_step, 0)

    for arr, base, out in ((0, u_ref, y_out), (1, dy_ref, du_out)):
        for part in PAIR:
            hops["left2", arr, part].wait_recv()
            hops["right2", arr, part].wait_recv()
            rows_at = pl.ds(part * half, half)
            val = base[rows_at].astype(jnp.float32) + total[arr, 1, rows_at] + inbox2[arr, 0, part].astype(jnp.float32) + inbox2[arr, 1, part].astype(jnp.float32)
            if arr == 1:
                val = val + du_router[part * half:(part + 1) * half]
            out[rows_at] = val.astype(jnp.bfloat16)
    wait_all(sends)
    for copy in pending.values():
        copy.wait()

    def drain(step, carry):
        dg_copy(step).wait_send()
        dl_copy(step).wait_send()
        return carry

    each_other(count, drain)


def reduce_call(mesh, y_part, du_part, all_rows, acts, dg_tiles, u_loc, dy_loc, wr_t, prob_t):
    etp_size, ep_size = mesh.shape["etp"], mesh.shape["ep"]
    tok, d_model = u_loc.shape
    count, ring, half = etp_size * ep_size, ep_size // 2, tok // 2
    assert ring == 4 and etp_size == 4
    shape5 = (ring, 2, etp_size, tok, d_model)
    vmem = pl.BlockSpec(memory_space=pltpu.VMEM)
    hbm = pl.BlockSpec(memory_space=pl.ANY)
    bf16, f32 = jnp.bfloat16, jnp.float32
    dma = pltpu.SemaphoreType.DMA
    return pl.pallas_call(
        functools.partial(reduce_kernel, etp_size),
        out_shape=(jax.ShapeDtypeStruct((tok, d_model), bf16), jax.ShapeDtypeStruct((tok, d_model), bf16), jax.ShapeDtypeStruct(wr_t.shape, f32)) + (jax.ShapeDtypeStruct((acts.shape[2], d_model), f32),) * 3,
        in_specs=[hbm, hbm, hbm, hbm, vmem, vmem, vmem, vmem, vmem],
        out_specs=(vmem, vmem, vmem, hbm, hbm, hbm),
        scratch_shapes=[
            pltpu.VMEM((2, 4, 4, tok, d_model), bf16),
            pltpu.VMEM((2, 4, 4, tok, d_model), bf16),
            pltpu.VMEM((2, 4, tok, d_model), bf16),
            pltpu.VMEM((2, 2, 4, tok, d_model), bf16),
            pltpu.VMEM((2, 2, tok, d_model), f32),
            pltpu.VMEM((2, 3, tok, d_model), bf16),
            pltpu.VMEM((2, 2, half, d_model), bf16),
            pltpu.VMEM((2, 2, 2, half, d_model), bf16),
            pltpu.VMEM((2, count * tok, d_model), bf16),
            pltpu.VMEM(acts.shape, bf16),
            pltpu.VMEM((2, 256, d_model), f32),
            pltpu.VMEM((count, 8, 128), f32),
            pltpu.VMEM((count, wr_t.shape[0], 128), bf16),
            pltpu.VMEM((wr_t.shape[0], 128), bf16),
            dma((3, 4)), dma((3,)), dma((2,)), dma((48,)), dma((48,)), dma((count,)), dma((count,)), dma((count,)), dma((count,)),
        ],
        compiler_params=pltpu.CompilerParams(collective_id=1, has_side_effects=True, vmem_limit_bytes=62 * 1024 * 1024),
        name="reduce_back",
    )(y_part.reshape(shape5), du_part.reshape(shape5), all_rows, acts, dg_tiles, u_loc, dy_loc, wr_t, prob_t)


SITES = tuple((tuple(map(int, two[:PAIR.stop])), tuple(map(int, two[PAIR.stop:]))) for two in "0003-1030-0102-3313-3111-2023-3212-2122".split("-"))
UP_SET = (0, 1)


def pick(idx, table):
    out = jnp.int32(table[0])
    for pos in range(1, len(table)):
        out = jnp.where(idx == pos, jnp.int32(table[pos]), out)
    return out


def gather_kernel(etp_size, ring, width, u_ref, dy_ref, ids_ref, wr_ref, w1_hbm, w3_hbm, w2_hbm,
                  y_hbm, du_hbm, all_hbm, act_hbm, dg_out, prob_out,
                  rows, w1, w3, w2, w1_t, w3_t, w2_t, y_buf, du_buf, act_buf, gate_out, gate_in,
                  w_sem, out_sem, keep_sem, send_sem, near_sem, half_sem, peer_sem, gate_send, gate_recv):
    ep, etp = lax.axis_index("ep"), lax.axis_index("etp")
    col, core = ep // 2, ep % 2
    lin = ep * etp_size + etp
    count = ring * 2 * etp_size
    tok, d_model = u_ref.shape
    half = tok // 2
    experts = wr_ref.shape[0]
    local_exp = experts // (2 * ring)
    bf16, f32 = jnp.bfloat16, jnp.float32

    w_copies = [pltpu.make_async_copy(src, dst, w_sem.at[pos]) for pos, (src, dst) in enumerate(((w1_hbm, w1), (w3_hbm, w3), (w2_hbm, w2)))]
    for copy in w_copies:
        copy.start()

    barrier = pltpu.get_barrier_semaphore()

    def other(step):
        dest = lax.rem(lin + step, count)
        return {"ep": dest // etp_size, "etp": lax.rem(dest, etp_size)}, dest

    def greet(step, carry):
        pl.semaphore_signal(barrier, inc=1, device_id=other(step)[0], device_id_type=MESH)
        return carry

    each_other(count, greet)
    logit = lax.dot_general(wr_ref[...], u_ref[...], (((1,), (1,)), ((), ())), preferred_element_type=f32)
    top = jnp.max(logit, axis=0, keepdims=True)
    expo = jnp.exp(logit - top)
    prob = expo / jnp.sum(expo, axis=0, keepdims=True)
    prob_out[...] = jnp.zeros_like(prob_out)
    prob_out[:, :tok] = prob
    ids = ids_ref[...]
    expert_at = lax.broadcasted_iota(jnp.int32, (experts, tok), 0)
    hot = expert_at == ids[0:1]
    for choice in range(1, ids.shape[0]):
        hot = hot | (expert_at == ids[choice:choice + 1])
    gate = jnp.where(hot, prob, 0.0)
    gate_out[...] = jnp.zeros_like(gate_out)
    for group in range(2 * ring):
        gate_out[group, :local_exp, :tok] = gate[group * local_exp:(group + 1) * local_exp]

    pl.semaphore_wait(barrier, count - 1)

    def at_x(step):
        return {"ep": lax.rem(col + step, ring) * 2 + core, "etp": etp}

    def at_y(step):
        return {"ep": ep, "etp": lax.rem(etp + step, etp_size)}

    along_first = (at_y, at_x)
    along_second = (at_x, at_y)
    partner = {"ep": col * 2 + 1 - core, "etp": etp}

    def spot(arr, first, second):
        rel_x, rel_y = (second, first) if arr == 0 else (first, second)
        return lax.rem(col + rel_x, ring), lax.rem(etp + rel_y, etp_size)

    def block(arr, first, second):
        x_at, y_at = spot(arr, first, second)
        return rows.at[arr, x_at, y_at, core]

    sends = []

    def send(src, dst, recv_sem, device):
        slot = len(sends)
        copy = pltpu.make_async_remote_copy(src, dst, send_sem.at[slot], recv_sem, device_id=device, device_id_type=MESH)
        copy.start()
        sends.append(src.shape[0])

    def landed(ref, sem):
        pltpu.make_async_copy(ref, ref, sem).wait()

    def to_second(arr, first, src):
        dst = block(arr, first, 0)
        send(src, dst, near_sem.at[arr, first, 3], along_second[arr](1))
        send(src, dst, near_sem.at[arr, first, 1], along_second[arr](3))

    def to_peer(arr, first, second, src):
        send(src, block(arr, first, second), peer_sem.at[arr, first, second], partner)

    def first_own(arr):
        src = (u_ref, dy_ref)[arr]
        dst = block(arr, 0, 0)
        send(src, dst, near_sem.at[arr, 3, 0], along_first[arr](1))
        send(src, dst, near_sem.at[arr, 1, 0], along_first[arr](3))
        to_peer(arr, 0, 0, src)

    def second_own(arr):
        to_second(arr, 0, (u_ref, dy_ref)[arr])

    def event_first(arr, first):
        ref = block(arr, first, 0)
        landed(ref, near_sem.at[arr, first, 0])
        part = 0 if first == 3 else 1
        piece = ref.at[pl.ds(part * half, half)]
        send(piece, piece, half_sem.at[arr, part], along_first[arr](1 if first == 3 else 3))
        to_peer(arr, first, 0, ref)
        to_second(arr, first, ref)

    def event_far(arr):
        ref = block(arr, 2, 0)
        for part in PAIR:
            landed(ref.at[pl.ds(part * half, half)], half_sem.at[arr, part])
        to_peer(arr, 2, 0, ref)
        to_second(arr, 2, ref)

    def event_near(arr, first):
        for second in (3, 1):
            ref = block(arr, first, second)
            landed(ref, near_sem.at[arr, first, second])
            if (second == 3) == (first in UP_SET):
                send(ref, ref, near_sem.at[arr, first, 2], along_second[arr](1 if second == 3 else 3))
            to_peer(arr, first, second, ref)

    def event_end(arr, first):
        ref = block(arr, first, 2)
        landed(ref, near_sem.at[arr, first, 2])
        to_peer(arr, first, 2, ref)

    def gate_copy(step):
        device, dest = other(step)
        return pltpu.make_async_remote_copy(gate_out.at[dest // etp_size], gate_in.at[lin], gate_send.at[step], gate_recv.at[lin], device_id=device, device_id_type=MESH)

    def start_gate(step, carry):
        gate_copy(step).start()
        return carry

    each_other(count, start_gate)
    gate_in[lin] = gate_out[ep]

    first_own(0)
    first_own(1)
    second_own(1)
    second_own(0)
    for arr, ref in enumerate((u_ref, dy_ref)):
        rows[arr, col, etp, core] = ref[...]

    lane_tile = 128
    for copy in w_copies:
        copy.wait()

    def flip(pos, carry):
        span = pl.ds(pl.multiple_of(pos * lane_tile, lane_tile), lane_tile)
        for src, dst in ((w1, w1_t), (w3, w3_t), (w2, w2_t)):
            dst[span, :] = src[:, span].T
        return carry

    lax.fori_loop(0, d_model // lane_tile, flip, 0)

    def wait_gate(step, carry):
        src = lax.rem(lin + step, count)
        landed(gate_in.at[src], gate_recv.at[src])
        return carry

    for first in (3, 1):
        for arr in PAIR:
            event_first(arr, first)

    def peer_wait(arr, site):
        first, second = (site[1], site[0]) if arr == 0 else (site[0], site[1])
        x_at, y_at = spot(arr, first, second)
        landed(rows.at[arr, x_at, y_at, 1 - core], peer_sem.at[arr, first, second])

    def event_gate():
        each_other(count, wait_gate)

    def both(event, *args):
        return [(event, (arr,) + args) for arr in PAIR]

    plan = {
        (0, 1): [(event_gate, ())] + both(event_near, 0),
        (0, 2): both(event_far),
        (1, 1): both(event_near, 3),
        (2, 0): both(event_end, 0),
        (2, 2): both(event_near, 1),
        (3, 2): both(event_near, 2),
        (4, 1): both(event_end, 3),
        (5, 1): both(event_end, 1) + both(event_end, 2),
    }

    def run_events(unit, point):
        for pos in range(len(SITES)):
            todo = list(plan.get((pos, point), []))
            if point < 2:
                todo += [(peer_wait, (point, site)) for site in SITES[pos]]
            if todo:
                @pl.when(unit == pos)
                def _():
                    for event, args in todo:
                        event(*args)

    def out_copies(slot, sites):
        copies = []
        for pos, (x_at, y_at) in enumerate(sites):
            base = pos * 2
            copies.append(pltpu.make_async_copy(y_buf.at[slot, pl.ds(base, 2)], y_hbm.at[x_at, :, y_at], out_sem.at[slot, pos, 0]))
            copies.append(pltpu.make_async_copy(du_buf.at[slot, pl.ds(base, 2)], du_hbm.at[x_at, :, y_at], out_sem.at[slot, pos, 1]))
            for kind in range(3):
                copies.append(pltpu.make_async_copy(act_buf.at[slot, kind, pl.ds(base, 2)], act_hbm.at[kind, x_at, y_at], out_sem.at[slot, pos, 2 + kind]))
        return copies

    def sites_of(unit):
        out = []
        for pos in PAIR:
            rel_x = pick(unit, [entry[pos][0] for entry in SITES])
            rel_y = pick(unit, [entry[pos][1] for entry in SITES])
            out.append((lax.rem(col + rel_x, ring), lax.rem(etp + rel_y, etp_size)))
        return out

    def load(arr, sites):
        return jnp.concatenate([rows[arr, x_at, y_at].reshape(2 * tok, d_model) for x_at, y_at in sites], axis=0)

    def mm(lhs, rhs):
        return jnp.dot(lhs, rhs, preferred_element_type=f32)

    def unit_step(unit, carry):
        slot = lax.rem(unit, 2)
        sites = sites_of(unit)
        run_events(unit, 0)

        @pl.when(unit >= 2)
        def _():
            for copy in out_copies(slot, sites):
                copy.wait()

        x_rows = load(0, sites)
        h1 = mm(x_rows, w1_t[...]).astype(bf16).astype(f32)
        h3 = mm(x_rows, w3_t[...]).astype(bf16).astype(f32)
        run_events(unit, 1)
        for arr in PAIR:
            for pos, (x_at, y_at) in enumerate(sites):
                pltpu.make_async_copy(rows.at[arr, x_at, y_at], all_hbm.at[arr, x_at, y_at], keep_sem.at[slot, arr, pos]).start()
        q = mm(load(1, sites), w2_t[...])
        cols = []
        lins = []
        for x_at, y_at in sites:
            for side in PAIR:
                src = (x_at * 2 + side) * etp_size + y_at
                lins.append(src)
                cols.append(gate_in[src].T[:tok])
        gate_cols = jnp.concatenate(cols, axis=0)
        lane = lax.broadcasted_iota(jnp.int32, q.shape, 1)
        wide = jnp.broadcast_to(gate_cols[:, local_exp - 1:local_exp], q.shape)
        for pos in range(local_exp - 2, -1, -1):
            wide = jnp.where(lane < (pos + 1) * width, gate_cols[:, pos:pos + 1], wide)
        live = wide > 0
        sig = jax.nn.sigmoid(h1)
        silu = h1 * sig
        act = jnp.where(live, (silu * h3).astype(bf16).astype(f32), 0.0)
        ga = (wide * act).astype(bf16)
        da = (wide * q).astype(bf16).astype(f32)
        dh1 = jnp.where(live, da * h3 * sig * (1.0 + h1 * (1.0 - sig)), 0.0).astype(bf16)
        dh3 = jnp.where(live, da * silu, 0.0).astype(bf16)
        prod = act * q
        dg_wide = jnp.zeros((prod.shape[0], lane_tile), f32)
        lane_s = lax.broadcasted_iota(jnp.int32, dg_wide.shape, 1)
        for pos in range(local_exp):
            total = jnp.zeros_like(dg_wide)
            for tile in range(pos * width // lane_tile, -(-(pos + 1) * width // lane_tile)):
                piece = prod[:, tile * lane_tile:(tile + 1) * lane_tile]
                low, high = pos * width - tile * lane_tile, (pos + 1) * width - tile * lane_tile
                if low > 0:
                    piece = jnp.where(lane_s >= low, piece, 0.0)
                if high < lane_tile:
                    piece = jnp.where(lane_s < high, piece, 0.0)
                total = total + piece
            dg_wide = jnp.where(lane_s == pos, jnp.sum(total, axis=1, keepdims=True), dg_wide)
        for pos, src in enumerate(lins):
            dg_out[src] = jnp.concatenate([dg_wide[pos * tok:(pos + 1) * tok].T[:8], jnp.zeros((8, lane_tile - tok), f32)], axis=1)
        for kind, val in enumerate((dh1, dh3, ga)):
            act_buf[slot, kind] = val.reshape(4, tok, val.shape[1])
        run_events(unit, 2)
        y_buf[slot] = mm(act_buf[slot, 2].reshape(4 * tok, -1), w2[...]).astype(bf16).reshape(4, tok, d_model)
        dx = mm(act_buf[slot, 0].reshape(4 * tok, -1), w1[...]) + mm(act_buf[slot, 1].reshape(4 * tok, -1), w3[...])
        du_buf[slot] = dx.astype(bf16).reshape(4, tok, d_model)
        for copy in out_copies(slot, sites):
            copy.start()
        for arr in PAIR:
            for pos, (x_at, y_at) in enumerate(sites):
                pltpu.make_async_copy(rows.at[arr, x_at, y_at], all_hbm.at[arr, x_at, y_at], keep_sem.at[slot, arr, pos]).wait()
        return carry

    units = len(SITES)
    lax.fori_loop(0, units, unit_step, 0)
    for unit in (units - 2, units - 1):
        for copy in out_copies(unit % 2, sites_of(unit)):
            copy.wait()
    for slot, size in enumerate(sends):
        ref = rows.at[0, 0, 0, 0, pl.ds(0, size)]
        landed(ref, send_sem.at[slot])

    def drain(step, carry):
        gate_copy(step).wait_send()
        return carry

    each_other(count, drain)


def gather_call(mesh, u_loc, dy_loc, ids_t, wr_t, w1, w3, w2):
    etp_size, ep_size = mesh.shape["etp"], mesh.shape["ep"]
    tok, d_model = u_loc.shape
    experts, inner = wr_t.shape[0], w1.shape[0]
    count, ring = etp_size * ep_size, ep_size // 2
    assert ring == 4 and etp_size == 4
    width = inner // (experts // ep_size)
    vmem = pl.BlockSpec(memory_space=pltpu.VMEM)
    hbm = pl.BlockSpec(memory_space=pl.ANY)
    bf16, f32 = jnp.bfloat16, jnp.float32
    dma = pltpu.SemaphoreType.DMA
    part = jax.ShapeDtypeStruct((ring, 2, etp_size, tok, d_model), bf16)
    return pl.pallas_call(
        functools.partial(gather_kernel, etp_size, ring, width),
        out_shape=(part, part, jax.ShapeDtypeStruct((2, ring, etp_size, 2, tok, d_model), bf16), jax.ShapeDtypeStruct((3, ring, etp_size, 2, tok, inner), bf16),
                   jax.ShapeDtypeStruct((count, 8, 128), f32), jax.ShapeDtypeStruct((experts, 128), f32)),
        in_specs=[vmem, vmem, vmem, vmem, hbm, hbm, hbm],
        out_specs=(hbm, hbm, hbm, hbm, vmem, vmem),
        scratch_shapes=[
            pltpu.VMEM((2, ring, etp_size, 2, tok, d_model), bf16),
            pltpu.VMEM((inner, d_model), bf16), pltpu.VMEM((inner, d_model), bf16), pltpu.VMEM((inner, d_model), bf16),
            pltpu.VMEM((d_model, inner), bf16), pltpu.VMEM((d_model, inner), bf16), pltpu.VMEM((d_model, inner), bf16),
            pltpu.VMEM((2, 4, tok, d_model), bf16), pltpu.VMEM((2, 4, tok, d_model), bf16), pltpu.VMEM((2, 3, 4, tok, inner), bf16),
            pltpu.VMEM((ep_size, 8, 128), f32), pltpu.VMEM((count, 8, 128), f32),
            dma((3,)), dma((2, 2, 5)), dma((2, 2, 2)), dma((72,)), dma((2, 4, 4)), dma((2, 2)), dma((2, 4, 4)), dma((count,)), dma((count,)),
        ],
        compiler_params=pltpu.CompilerParams(collective_id=0, has_side_effects=True, vmem_limit_bytes=60 * 1024 * 1024),
        name="gather_experts",
    )(u_loc, dy_loc, ids_t, wr_t, w1, w3, w2)


def solution(mesh):
    tok_spec = P(("dp", "ep", "etp"), None)
    col_spec = P("ep", None, "etp")
    row_spec = P("ep", "etp", None)
    in_specs = (tok_spec, tok_spec, tok_spec, P(None, None), col_spec, col_spec, row_spec)
    out_specs = (tok_spec, tok_spec, P(("dp", "ep"), None, "etp"), P(("dp", "ep"), None, "etp"), P(("dp", "ep"), "etp", None), P("dp", None))

    def device_step(u_loc, dy_loc, ids_loc, w_router, w_gate, w_up, w_down):
        local_exp, d_model, width = w_gate.shape
        inner = local_exp * width
        w1 = jnp.swapaxes(w_gate, 1, 2).reshape(inner, d_model)
        w3 = jnp.swapaxes(w_up, 1, 2).reshape(inner, d_model)
        w2 = w_down.reshape(inner, d_model)
        y_part, du_part, both_all, acts, dg_tiles, prob_t = gather_call(mesh, u_loc, dy_loc, ids_loc.T, w_router.T, w1, w3, w2)
        both_all = both_all.reshape(2, -1, d_model)
        acts = acts.reshape(3, -1, inner)
        y_loc, du_loc, dwr_t, dw1, dw3, dw2 = reduce_call(mesh, y_part, du_part, both_all, acts, dg_tiles, u_loc, dy_loc, w_router.T, prob_t)
        unfold = lambda d: jnp.swapaxes(d.reshape(local_exp, width, d_model), 1, 2)
        return y_loc, du_loc, unfold(dw1), unfold(dw3), dw2.reshape(local_exp, width, d_model), dwr_t.T

    return jax.shard_map(device_step, mesh=mesh, in_specs=in_specs, out_specs=out_specs, check_vma=False)
```

```python
import functools

import jax
import jax.numpy as jnp
from jax import lax
from jax.experimental import pallas as pl
from jax.experimental.pallas import tpu as pltpu
from jax.sharding import PartitionSpec as P

MESH = pl.DeviceIdType.MESH
PAIR = range(2)


def each_other(count, step):
    lax.fori_loop(1, count, step, 0)


SITES = tuple((tuple(map(int, two[:PAIR.stop])), tuple(map(int, two[PAIR.stop:]))) for two in "0003-0110-3033-1331-1102-2023-2112-3222".split("-"))
UP_SET = (0, 1)


def pick(idx, table):
    out = jnp.int32(table[0])
    for pos in range(1, len(table)):
        out = jnp.where(idx == pos, jnp.int32(table[pos]), out)
    return out


def block_kernel(etp_size, ring, width, u_ref, dy_ref, ids_ref, wr_ref, w1_hbm, w3_hbm, w2_hbm,
                 y_out, du_out, dwr_out, dw1_hbm, dw3_hbm, dw2_hbm, act_hbm,
                 rows, w1, w3, w2, wide, y_buf, du_buf, act_buf, h_buf, gate_out, gate_in, dg_out, prob_ref,
                 mine, peer, relay, inbox, total, stage, relay2, inbox2, dw_buf, dg_in, dl_in, dl_out,
                 w_sem, act_sem, send_sem, near_sem, half_sem, peer_sem, gate_send, gate_recv,
                 swap_send, swap_sem, back_send, back_recv, load_sem, dw_sem, dg_send, dg_recv, dl_send, dl_recv):
    ep, etp = lax.axis_index("ep"), lax.axis_index("etp")
    col, core = ep // 2, ep % 2
    lin = ep * etp_size + etp
    count = ring * 2 * etp_size
    tok, d_model = u_ref.shape
    half = tok // 2
    experts = wr_ref.shape[0]
    local_exp = experts // (2 * ring)
    bf16, f32 = jnp.bfloat16, jnp.float32

    w_copies = [pltpu.make_async_copy(src, dst, w_sem.at[pos]) for pos, (src, dst) in enumerate(((w1_hbm, w1), (w3_hbm, w3), (w2_hbm, w2)))]
    for copy in w_copies:
        copy.start()

    barrier = pltpu.get_barrier_semaphore()

    def other(step):
        dest = lax.rem(lin + step, count)
        return {"ep": dest // etp_size, "etp": lax.rem(dest, etp_size)}, dest

    def greet(step, carry):
        pl.semaphore_signal(barrier, inc=1, device_id=other(step)[0], device_id_type=MESH)
        return carry

    each_other(count, greet)
    logit = lax.dot_general(wr_ref[...], u_ref[...], (((1,), (1,)), ((), ())), preferred_element_type=f32)
    top = jnp.max(logit, axis=0, keepdims=True)
    expo = jnp.exp(logit - top)
    prob = expo / jnp.sum(expo, axis=0, keepdims=True)
    prob_ref[...] = jnp.zeros_like(prob_ref)
    prob_ref[:, :tok] = prob
    ids = ids_ref[...]
    expert_at = lax.broadcasted_iota(jnp.int32, (experts, tok), 0)
    hot = expert_at == ids[0:1]
    for choice in range(1, ids.shape[0]):
        hot = hot | (expert_at == ids[choice:choice + 1])
    gate = jnp.where(hot, prob, 0.0)
    gate_out[...] = jnp.zeros_like(gate_out)
    for group in range(2 * ring):
        gate_out[group, :local_exp, :tok] = gate[group * local_exp:(group + 1) * local_exp]

    pl.semaphore_wait(barrier, count - 1)

    def at_x(step):
        return {"ep": lax.rem(col + step, ring) * 2 + core, "etp": etp}

    def at_y(step):
        return {"ep": ep, "etp": lax.rem(etp + step, etp_size)}

    along_first = (at_y, at_x)
    along_second = (at_x, at_y)
    partner = {"ep": col * 2 + 1 - core, "etp": etp}

    def spot(arr, first, second):
        rel_x, rel_y = (second, first) if arr == 0 else (first, second)
        return lax.rem(col + rel_x, ring), lax.rem(etp + rel_y, etp_size)

    def block(arr, first, second):
        x_at, y_at = spot(arr, first, second)
        return rows.at[arr, x_at, y_at, core]

    sends = []

    def send(src, dst, recv_sem, device):
        slot = len(sends)
        copy = pltpu.make_async_remote_copy(src, dst, send_sem.at[slot], recv_sem, device_id=device, device_id_type=MESH)
        copy.start()
        sends.append(src.shape[0])

    def landed(ref, sem):
        pltpu.make_async_copy(ref, ref, sem).wait()

    def to_second(arr, first, src):
        dst = block(arr, first, 0)
        send(src, dst, near_sem.at[arr, first, 3], along_second[arr](1))
        send(src, dst, near_sem.at[arr, first, 1], along_second[arr](3))

    def to_peer(arr, first, second, src):
        send(src, block(arr, first, second), peer_sem.at[arr, first, second], partner)

    def first_own(arr):
        src = (u_ref, dy_ref)[arr]
        dst = block(arr, 0, 0)
        send(src, dst, near_sem.at[arr, 3, 0], along_first[arr](1))
        send(src, dst, near_sem.at[arr, 1, 0], along_first[arr](3))
        to_peer(arr, 0, 0, src)

    def second_own(arr):
        to_second(arr, 0, (u_ref, dy_ref)[arr])

    def event_first(arr, first):
        ref = block(arr, first, 0)
        landed(ref, near_sem.at[arr, first, 0])
        part = 0 if first == 3 else 1
        piece = ref.at[pl.ds(part * half, half)]
        send(piece, piece, half_sem.at[arr, part], along_first[arr](1 if first == 3 else 3))
        to_peer(arr, first, 0, ref)
        to_second(arr, first, ref)

    def event_far(arr):
        ref = block(arr, 2, 0)
        for part in PAIR:
            landed(ref.at[pl.ds(part * half, half)], half_sem.at[arr, part])
        to_peer(arr, 2, 0, ref)
        to_second(arr, 2, ref)

    def event_relay(arr, first):
        second = 3 if first in UP_SET else 1
        ref = block(arr, first, second)
        send(ref, ref, near_sem.at[arr, first, 2], along_second[arr](4 - second))

    def event_near(arr, first):
        for second in (3, 1):
            ref = block(arr, first, second)
            landed(ref, near_sem.at[arr, first, second])
            to_peer(arr, first, second, ref)

    def event_end(arr, first):
        ref = block(arr, first, 2)
        landed(ref, near_sem.at[arr, first, 2])
        to_peer(arr, first, 2, ref)

    def gate_copy(step):
        device, dest = other(step)
        return pltpu.make_async_remote_copy(gate_out.at[dest // etp_size], gate_in.at[lin], gate_send.at[step], gate_recv.at[lin], device_id=device, device_id_type=MESH)

    def start_gate(step, carry):
        gate_copy(step).start()
        return carry

    each_other(count, start_gate)
    gate_in[lin] = gate_out[ep]

    first_own(0)
    first_own(1)
    second_own(1)
    second_own(0)
    for arr, ref in enumerate((u_ref, dy_ref)):
        rows[arr, col, etp, core] = ref[...]

    lane_tile = 128
    for copy in w_copies:
        copy.wait()

    def flip(pos, carry):
        span = pl.ds(pl.multiple_of(pos * lane_tile, lane_tile), lane_tile)
        for src, dst in ((w1, wide.at[0]), (w3, wide.at[1]), (w2, wide.at[2])):
            dst[span, :] = src[:, span].T
        return carry

    lax.fori_loop(0, d_model // lane_tile, flip, 0)

    def wait_gate(step, carry):
        src = lax.rem(lin + step, count)
        landed(gate_in.at[src], gate_recv.at[src])
        return carry

    for first in (3, 1):
        for arr in PAIR:
            event_first(arr, first)

    def peer_wait(arr, site):
        first, second = (site[1], site[0]) if arr == 0 else (site[0], site[1])
        x_at, y_at = spot(arr, first, second)
        landed(rows.at[arr, x_at, y_at, 1 - core], peer_sem.at[arr, first, second])

    def event_gate():
        each_other(count, wait_gate)

    def both(event, *args):
        return [(event, (arr,) + args) for arr in PAIR]

    spots = ((col, etp), (etp, col))
    back_sends = []
    back_slot = {}

    def back(key, src, dst, device):
        slot = back_slot.setdefault(key, len(back_slot))
        copy = pltpu.make_async_remote_copy(src, dst, back_send.at[slot], back_recv.at[slot], device_id=device, device_id_type=MESH)
        copy.start()
        back_sends.append((slot, src.shape[0]))

    def arrive(key, ref):
        landed(ref, back_recv.at[back_slot[key]])

    def cell(ref, arr, first, sub):
        return ref.at[arr, lax.rem(spots[arr][0] + first, ring), lax.rem(spots[arr][1] + sub, ring)]

    def value(arr, first, sub):
        landed(cell(peer, arr, first, sub), swap_sem.at[arr, first, sub])
        return cell(mine, arr, first, sub)[...].astype(f32) + cell(peer, arr, first, sub)[...].astype(f32)

    def put(arr, first, sub, val):
        ref = cell(mine, arr, first, sub)
        ref[...] = val.astype(bf16)
        return ref

    far_slot = {2: 0, 1: 1, 3: 2, 0: 3}

    def back_far(arr, sub):
        device = along_stage(arr, sub in (2, 1))
        back(("far", arr, sub), put(arr, 2, sub, value(arr, 2, sub)), relay.at[arr, far_slot[sub]], device)

    def along_stage(arr, right):
        return along_second[arr](1 if right else 3)

    def back_direct(arr, sub):
        right = sub in (3, 0)
        first = 1 if right else 3
        back(("left" if right else "right", arr, sub), put(arr, first, sub, value(arr, first, sub)), inbox.at[arr, 0 if right else 1, sub], along_stage(arr, right))

    def back_relay(arr, sub):
        right = sub in (2, 1)
        first = 1 if right else 3
        incoming = relay.at[arr, far_slot[sub]]
        arrive(("far", arr, sub), incoming)
        val = value(arr, first, sub) + incoming[...].astype(f32)
        back(("left" if right else "right", arr, sub), put(arr, first, sub, val), inbox.at[arr, 0 if right else 1, sub], along_stage(arr, right))

    plan = {
        (0, 1): [(event_gate, ())] + both(event_near, 0),
        (0, 2): both(event_far) + both(event_relay, 0),
        (1, 2): both(event_near, 3) + both(event_relay, 3),
        (2, 1): both(event_near, 1) + both(event_relay, 1),
        (3, 1): both(event_near, 2) + both(event_relay, 2),
        (4, 0): both(back_direct, 0),
        (4, 1): both(event_end, 0),
        (4, 2): both(event_end, 3) + both(back_direct, 3),
        (4, 3): both(back_direct, 1),
        (5, 1): both(event_end, 1) + both(event_end, 2),
        (5, 2): [(back_far, (1, 0))],
        (6, 1): both(back_far, 0)[:1] + [(back_far, (0, 3)), (back_direct, (1, 2))],
        (7, 1): both(back_far, 1),
    }

    def run_events(unit, point):
        for pos in range(len(SITES)):
            todo = list(plan.get((pos, point), []))
            if point < 2:
                todo += [(peer_wait, (point, site)) for site in SITES[pos]]
            if todo:
                @pl.when(unit == pos)
                def _():
                    for event, args in todo:
                        event(*args)

    def act_copies(sites):
        copies = []
        for pos, (x_at, y_at) in enumerate(sites):
            site = (x_at * etp_size + y_at) * 2 * tok
            for kind in range(3):
                copies.append(pltpu.make_async_copy(act_buf.at[kind, pl.ds(pos * 2 * tok, 2 * tok)], act_hbm.at[kind, pl.ds(pl.multiple_of(site, 2 * tok), 2 * tok)], act_sem.at[pos, kind]))
        return copies

    def swap_copies(slot, sites, rels):
        copies = []
        for pos, (x_at, y_at) in enumerate(sites):
            rel_x, rel_y = rels[pos]
            away = 2 * pos + 1 - core
            copies.append(pltpu.make_async_remote_copy(y_buf.at[slot, away], peer.at[0, x_at, y_at], swap_send.at[slot, pos, 0], swap_sem.at[0, rel_x, rel_y], device_id=partner, device_id_type=MESH))
            copies.append(pltpu.make_async_remote_copy(du_buf.at[slot, away], peer.at[1, y_at, x_at], swap_send.at[slot, pos, 1], swap_sem.at[1, rel_y, rel_x], device_id=partner, device_id_type=MESH))
        return copies

    def wait_swaps(slot):
        for pos in PAIR:
            landed(y_buf.at[0, 0], swap_send.at[slot, pos, 0])
            landed(du_buf.at[0, 0], swap_send.at[slot, pos, 1])

    def sites_of(unit):
        out = []
        rels = []
        for pos in PAIR:
            rel_x = pick(unit, [entry[pos][0] for entry in SITES])
            rel_y = pick(unit, [entry[pos][1] for entry in SITES])
            out.append((lax.rem(col + rel_x, ring), lax.rem(etp + rel_y, etp_size)))
            rels.append((rel_x, rel_y))
        return out, rels

    def load(arr, sites):
        return jnp.concatenate([rows[arr, x_at, y_at].reshape(2 * tok, d_model) for x_at, y_at in sites], axis=0)

    def mm(lhs, rhs):
        return jnp.dot(lhs, rhs, preferred_element_type=f32)

    def unit_step(unit, carry):
        slot = lax.rem(unit, 2)
        sites, rels = sites_of(unit)
        run_events(unit, 0)

        @pl.when(unit >= 2)
        def _():
            wait_swaps(slot)

        x_rows = load(0, sites)
        h_buf[0] = mm(x_rows, wide[0, :d_model]).astype(bf16)
        h_buf[1] = mm(x_rows, wide[1, :d_model]).astype(bf16)
        run_events(unit, 1)
        @pl.when(unit >= 1)
        def _():
            for copy in act_copies(sites):
                copy.wait()

        q = mm(load(1, sites), wide[2, :d_model])
        cols = []
        lins = []
        for x_at, y_at in sites:
            for side in PAIR:
                src = (x_at * 2 + side) * etp_size + y_at
                lins.append(src)
                cols.append(gate_in[src].T[:tok])
        gate_cols = jnp.concatenate(cols, axis=0)
        lane = lax.broadcasted_iota(jnp.int32, q.shape, 1)
        spread = jnp.broadcast_to(gate_cols[:, local_exp - 1:local_exp], q.shape)
        for pos in range(local_exp - 2, -1, -1):
            spread = jnp.where(lane < (pos + 1) * width, gate_cols[:, pos:pos + 1], spread)
        live = spread > 0
        h1 = jnp.where(live, h_buf[0].astype(f32), 0.0)
        h3 = jnp.where(live, h_buf[1].astype(f32), 0.0)
        sig = jax.nn.sigmoid(h1)
        silu = h1 * sig
        act = (silu * h3).astype(bf16).astype(f32)
        ga = (spread * act).astype(bf16)
        act_buf[2] = ga
        y_buf[slot] = mm(ga, w2[...]).astype(bf16).reshape(4, tok, d_model)
        q = jnp.where(live, q, 0.0)
        da = (spread * q).astype(bf16).astype(f32)
        act_buf[0] = (da * h3 * (sig + silu * (1.0 - sig))).astype(bf16)
        act_buf[1] = (da * silu).astype(bf16)
        prod = act * q
        dg_wide = jnp.zeros((prod.shape[0], lane_tile), f32)
        lane_s = lax.broadcasted_iota(jnp.int32, dg_wide.shape, 1)
        for pos in range(local_exp):
            part_sum = jnp.zeros_like(dg_wide)
            for tile in range(pos * width // lane_tile, -(-(pos + 1) * width // lane_tile)):
                piece = prod[:, tile * lane_tile:(tile + 1) * lane_tile]
                low, high = pos * width - tile * lane_tile, (pos + 1) * width - tile * lane_tile
                if low > 0:
                    piece = jnp.where(lane_s >= low, piece, 0.0)
                if high < lane_tile:
                    piece = jnp.where(lane_s < high, piece, 0.0)
                part_sum = part_sum + piece
            dg_wide = jnp.where(lane_s == pos, jnp.sum(part_sum, axis=1, keepdims=True), dg_wide)
        for pos, src in enumerate(lins):
            dg_out[src] = jnp.concatenate([dg_wide[pos * tok:(pos + 1) * tok].T[:8], jnp.zeros((8, lane_tile - tok), f32)], axis=1)
        run_events(unit, 2)
        run_events(unit, 3)
        dx = mm(act_buf[0], w1[...]) + mm(act_buf[1], w3[...])
        du_buf[slot] = dx.astype(bf16).reshape(4, tok, d_model)
        for copy in act_copies(sites) + swap_copies(slot, sites, rels):
            copy.start()
        for pos, (x_at, y_at) in enumerate(sites):
            mine[0, x_at, y_at] = y_buf[slot, 2 * pos + core]
            mine[1, y_at, x_at] = du_buf[slot, 2 * pos + core]
        return carry

    lax.fori_loop(0, len(SITES), unit_step, 0)

    def dg_copy(step):
        device, dest = other(step)
        return pltpu.make_async_remote_copy(dg_out.at[dest], dg_in.at[lin], dg_send.at[step], dg_recv.at[lin], device_id=device, device_id_type=MESH)

    def dl_copy(step):
        device, dest = other(step)
        return pltpu.make_async_remote_copy(dl_out, dl_in.at[lin], dl_send.at[step], dl_recv.at[lin], device_id=device, device_id_type=MESH)

    def start_dg(step, carry):
        dg_copy(step).start()
        return carry

    each_other(count, start_dg)
    dg_in[lin] = dg_out[lin]
    for copy in act_copies(sites_of(0)[0]):
        copy.wait()
    act_loads = [pltpu.make_async_copy(act_hbm.at[kind], wide.at[kind], load_sem.at[kind]) for kind in range(3)]
    for copy in act_loads:
        copy.start()
    dw_outs = (dw1_hbm, dw3_hbm, dw2_hbm)
    inner = dw1_hbm.shape[0]
    chunk = dw_buf.shape[1]
    chunks = inner // chunk
    pending = {}
    todo = list(range(3 * chunks))

    def dw_steps(number):
        for _ in range(number):
            index = todo.pop(0)
            kind, part = divmod(index, chunks)
            if part == 0:
                act_loads[kind].wait()
            slot = index % 2
            if slot in pending:
                pending[slot].wait()
            lhs = wide[kind, :, part * chunk:(part + 1) * chunk]
            rhs = rows[kind // 2].reshape(count * tok, d_model)
            dw_buf[slot] = lax.dot_general(lhs, rhs, (((0,), (0,)), ((), ())), preferred_element_type=f32)
            pending[slot] = pltpu.make_async_copy(dw_buf.at[slot], dw_outs[kind].at[pl.ds(part * chunk, chunk)], dw_sem.at[slot])
            pending[slot].start()

    back_far(0, 2)
    back_far(1, 2)
    back_far(1, 3)
    back_direct(0, 2)
    dw_steps(2)
    for arr, sub in ((0, 0), (1, 0), (0, 3), (0, 1), (1, 1)):
        back_relay(arr, sub)

    def wait_dg(step, carry):
        src = lax.rem(lin + step, count)
        landed(dg_in.at[src], dg_recv.at[src])
        return carry

    each_other(count, wait_dg)
    tiles = []
    for group in range(2 * ring):
        tile = dg_in[group * etp_size]
        for part in range(1, etp_size):
            tile = tile + dg_in[group * etp_size + part]
        tiles.append(tile[:local_exp])
    d_gate = jnp.concatenate(tiles, axis=0)
    prob_all = prob_ref[...]
    d_logit = prob_all * (d_gate - jnp.sum(prob_all * d_gate, axis=0, keepdims=True))
    dl_out[...] = d_logit.astype(bf16)
    dl_in[lin] = d_logit.astype(bf16)

    def start_dl(step, carry):
        dl_copy(step).start()
        return carry

    each_other(count, start_dl)
    dw_steps(4)
    for arr, sub in ((0, 2), (1, 2), (1, 3)):
        back_relay(arr, sub)
    dw_steps(4)

    def settle(arr, sub):
        arrive(("left", arr, sub), inbox.at[arr, 0, sub])
        arrive(("right", arr, sub), inbox.at[arr, 1, sub])
        return value(arr, 0, sub) + inbox[arr, 0, sub].astype(f32) + inbox[arr, 1, sub].astype(f32)

    def ship(key, arr, sub, part, val, dst, step):
        rows_at = pl.ds(part * half, half)
        stage[arr, sub - 1, rows_at] = val.astype(bf16)
        back(key, stage.at[arr, sub - 1, rows_at], dst, along_first[arr](step))

    for arr in PAIR:
        val = settle(arr, 1)
        ship(("left2", arr, 1), arr, 1, 1, val[half:], inbox2.at[arr, 0, 1], 1)
        total[arr, 0, :half] = val[:half]
    for arr in PAIR:
        val = settle(arr, 2)
        ship(("far2", arr, 0), arr, 2, 0, val[:half], relay2.at[arr, 0], 1)
        ship(("far2", arr, 1), arr, 2, 1, val[half:], relay2.at[arr, 1], 3)
    for arr in PAIR:
        val = settle(arr, 3)
        ship(("right2", arr, 0), arr, 3, 0, val[:half], inbox2.at[arr, 1, 0], 3)
        total[arr, 0, half:] = val[half:]
    dw_steps(2)
    for arr in PAIR:
        arrive(("far2", arr, 0), relay2.at[arr, 0])
        val = total[arr, 0, :half] + relay2[arr, 0].astype(f32)
        ship(("left2", arr, 0), arr, 1, 0, val, inbox2.at[arr, 0, 0], 1)
        arrive(("far2", arr, 1), relay2.at[arr, 1])
        val = total[arr, 0, half:] + relay2[arr, 1].astype(f32)
        ship(("right2", arr, 1), arr, 3, 1, val, inbox2.at[arr, 1, 1], 3)
    for arr in PAIR:
        total[arr, 1] = settle(arr, 0)

    def wait_dl(step, carry):
        src = lax.rem(lin + step, count)
        landed(dl_in.at[src], dl_recv.at[src])
        return carry

    each_other(count, wait_dl)
    du_router = lax.dot_general(dl_out[...], wr_ref[...], (((0,), (0,)), ((), ())), preferred_element_type=f32)[:tok]
    dwr_out[...] = jnp.zeros_like(dwr_out)

    def dwr_step(idx, carry):
        parts = []
        for pair in range(etp_size):
            low = dl_in[idx * 2 * etp_size + pair].astype(f32)
            high = dl_in[(idx * 2 + 1) * etp_size + pair].astype(f32)
            parts.append((low + pltpu.roll(high, tok, 1)).astype(bf16))
        dwr_out[...] += mm(jnp.concatenate(parts, axis=1), rows[0, idx].reshape(2 * etp_size * tok, d_model))
        return carry

    lax.fori_loop(0, ring, dwr_step, 0)
    dw_steps(len(todo))
    for part in PAIR:
        for arr, base, out in ((0, u_ref, y_out), (1, dy_ref, du_out)):
            arrive(("left2", arr, part), inbox2.at[arr, 0, part])
            arrive(("right2", arr, part), inbox2.at[arr, 1, part])
            rows_at = pl.ds(part * half, half)
            val = base[rows_at].astype(f32) + total[arr, 1, rows_at] + inbox2[arr, 0, part].astype(f32) + inbox2[arr, 1, part].astype(f32)
            if arr == 1:
                val = val + du_router[part * half:(part + 1) * half]
            out[rows_at] = val.astype(bf16)
    for slot in PAIR:
        wait_swaps(slot)
    for copy in pending.values():
        copy.wait()
    for slot, size in enumerate(sends):
        landed(rows.at[0, 0, 0, 0, pl.ds(0, size)], send_sem.at[slot])
    for slot, size in back_sends:
        landed(rows.at[0, 0, 0, 0, pl.ds(0, size)], back_send.at[slot])

    def drain(step, carry):
        gate_copy(step).wait_send()
        dg_copy(step).wait_send()
        dl_copy(step).wait_send()
        return carry

    each_other(count, drain)


def block_call(mesh, u_loc, dy_loc, ids_t, wr_t, w1, w3, w2):
    etp_size, ep_size = mesh.shape["etp"], mesh.shape["ep"]
    tok, d_model = u_loc.shape
    experts, inner = wr_t.shape[0], w1.shape[0]
    count, ring, half = etp_size * ep_size, ep_size // 2, tok // 2
    assert ring == 4 and etp_size == 4
    width = inner // (experts // ep_size)
    vmem = pl.BlockSpec(memory_space=pltpu.VMEM)
    hbm = pl.BlockSpec(memory_space=pl.ANY)
    bf16, f32 = jnp.bfloat16, jnp.float32
    dma = pltpu.SemaphoreType.DMA
    shape = jax.ShapeDtypeStruct
    quad = (2, ring, etp_size)
    return pl.pallas_call(
        functools.partial(block_kernel, etp_size, ring, width),
        out_shape=(shape((tok, d_model), bf16),) * 2 + (shape((experts, d_model), f32),) + (shape((inner, d_model), f32),) * 3 + (shape((3, count * tok, inner), bf16),),
        in_specs=[vmem] * 4 + [hbm] * 3,
        out_specs=(vmem,) * 3 + (hbm,) * 4,
        scratch_shapes=[
            pltpu.VMEM(quad + (2, tok, d_model), bf16),
            pltpu.VMEM((inner, d_model), bf16), pltpu.VMEM((inner, d_model), bf16), pltpu.VMEM((inner, d_model), bf16),
            pltpu.VMEM((3, count * tok, inner), bf16),
            pltpu.VMEM((2, 4, tok, d_model), bf16), pltpu.VMEM((2, 4, tok, d_model), bf16), pltpu.VMEM((3, 4 * tok, inner), bf16), pltpu.VMEM((2, 4 * tok, inner), bf16),
            pltpu.VMEM((ep_size, 8, 128), f32), pltpu.VMEM((count, 8, 128), f32), pltpu.VMEM((count, 8, 128), f32), pltpu.VMEM((experts, 128), f32),
            pltpu.VMEM(quad + (tok, d_model), bf16), pltpu.VMEM(quad + (tok, d_model), bf16),
            pltpu.VMEM((2, 4, tok, d_model), bf16),
            pltpu.VMEM((2, 2, 4, tok, d_model), bf16),
            pltpu.VMEM((2, 2, tok, d_model), f32),
            pltpu.VMEM((2, 3, tok, d_model), bf16),
            pltpu.VMEM((2, 2, half, d_model), bf16),
            pltpu.VMEM((2, 2, 2, half, d_model), bf16),
            pltpu.VMEM((2, 128, d_model), f32),
            pltpu.VMEM((count, 8, 128), f32),
            pltpu.VMEM((count, experts, 128), bf16),
            pltpu.VMEM((experts, 128), bf16),
            dma((3,)), dma((2, 3)), dma((72,)), dma(quad), dma((2, 2)), dma(quad), dma((count,)), dma((count,)),
            dma((2, 2, 2)), dma(quad), dma((48,)), dma((48,)), dma((3,)), dma((2,)), dma((count,)), dma((count,)), dma((count,)), dma((count,)),
        ],
        compiler_params=pltpu.CompilerParams(collective_id=0, has_side_effects=True, vmem_limit_bytes=67043328),
        name="moe_block",
    )(u_loc, dy_loc, ids_t, wr_t, w1, w3, w2)[:6]


def solution(mesh):
    tok_spec = P(("dp", "ep", "etp"), None)
    col_spec = P("ep", None, "etp")
    row_spec = P("ep", "etp", None)
    in_specs = (tok_spec, tok_spec, tok_spec, P(None, None), col_spec, col_spec, row_spec)
    out_specs = (tok_spec, tok_spec, P(("dp", "ep"), None, "etp"), P(("dp", "ep"), None, "etp"), P(("dp", "ep"), "etp", None), P("dp", None))

    def device_step(u_loc, dy_loc, ids_loc, w_router, w_gate, w_up, w_down):
        local_exp, d_model, width = w_gate.shape
        inner = local_exp * width
        w1 = jnp.swapaxes(w_gate, 1, 2).reshape(inner, d_model)
        w3 = jnp.swapaxes(w_up, 1, 2).reshape(inner, d_model)
        w2 = w_down.reshape(inner, d_model)
        y_loc, du_loc, dwr_t, dw1, dw3, dw2 = block_call(mesh, u_loc, dy_loc, ids_loc.T, w_router.T, w1, w3, w2)
        unfold = lambda d: jnp.swapaxes(d.reshape(local_exp, width, d_model), 1, 2)
        return y_loc, du_loc, unfold(dw1), unfold(dw3), dw2.reshape(local_exp, width, d_model), dwr_t.T

    return jax.shard_map(device_step, mesh=mesh, in_specs=in_specs, out_specs=out_specs, check_vma=False)
```

```python
import functools

import jax
import jax.numpy as jnp
from jax import lax
from jax.experimental import pallas as pl
from jax.experimental.pallas import tpu as pltpu
from jax.sharding import PartitionSpec as P

MESH = pl.DeviceIdType.MESH
PAIR = range(2)


def each_other(count, step):
    lax.fori_loop(1, count, step, 0)


SITES = tuple((tuple(map(int, two[:PAIR.stop])), tuple(map(int, two[PAIR.stop:]))) for two in "0003-0110-3033-1331-1102-2023-2112-3222".split("-"))
UP_SET = (0, 1)


def pick(idx, table):
    out = jnp.int32(table[0])
    for pos in range(1, len(table)):
        out = jnp.where(idx == pos, jnp.int32(table[pos]), out)
    return out


def block_kernel(etp_size, ring, width, u_ref, dy_ref, ids_ref, wr_ref, w1_hbm, w3_hbm, w2_hbm,
                 y_out, du_out, dwr_out, dw1_hbm, dw3_hbm, dw2_hbm, act_hbm,
                 rows, w1, w3, w2, wide, y_buf, du_buf, act_buf, h_buf, gate_out, gate_in, dg_out, prob_ref,
                 mine, peer, relay, inbox, total, stage, relay2, inbox2, dw_buf, dg_in, dl_in, dl_out,
                 w_sem, act_sem, send_sem, near_sem, half_sem, peer_sem, gate_send, gate_recv,
                 swap_send, swap_sem, back_send, back_recv, load_sem, dw_sem, dg_send, dg_recv, dl_send, dl_recv):
    ep, etp = lax.axis_index("ep"), lax.axis_index("etp")
    col, core = ep // 2, ep % 2
    lin = ep * etp_size + etp
    count = ring * 2 * etp_size
    tok, d_model = u_ref.shape
    half = tok // 2
    experts = wr_ref.shape[0]
    local_exp = experts // (2 * ring)
    bf16, f32 = jnp.bfloat16, jnp.float32

    w_copies = [pltpu.make_async_copy(src, dst, w_sem.at[pos]) for pos, (src, dst) in enumerate(((w1_hbm, w1), (w3_hbm, w3), (w2_hbm, w2)))]
    for copy in w_copies:
        copy.start()

    barrier = pltpu.get_barrier_semaphore()

    def other(step):
        dest = lax.rem(lin + step, count)
        return {"ep": dest // etp_size, "etp": lax.rem(dest, etp_size)}, dest

    def greet(step, carry):
        pl.semaphore_signal(barrier, inc=1, device_id=other(step)[0], device_id_type=MESH)
        return carry

    each_other(count, greet)
    logit = lax.dot_general(wr_ref[...], u_ref[...], (((1,), (1,)), ((), ())), preferred_element_type=f32)
    top = jnp.max(logit, axis=0, keepdims=True)
    expo = jnp.exp(logit - top)
    prob = expo / jnp.sum(expo, axis=0, keepdims=True)
    prob_ref[...] = jnp.zeros_like(prob_ref)
    prob_ref[:, :tok] = prob
    ids = ids_ref[...]
    expert_at = lax.broadcasted_iota(jnp.int32, (experts, tok), 0)
    hot = expert_at == ids[0:1]
    for choice in range(1, ids.shape[0]):
        hot = hot | (expert_at == ids[choice:choice + 1])
    gate = jnp.where(hot, prob, 0.0)
    gate_out[...] = jnp.zeros_like(gate_out)
    for group in range(2 * ring):
        gate_out[group, :local_exp, :tok] = gate[group * local_exp:(group + 1) * local_exp]

    pl.semaphore_wait(barrier, count - 1)

    def at_x(step):
        return {"ep": lax.rem(col + step, ring) * 2 + core, "etp": etp}

    def at_y(step):
        return {"ep": ep, "etp": lax.rem(etp + step, etp_size)}

    along_first = (at_y, at_x)
    along_second = (at_x, at_y)
    partner = {"ep": col * 2 + 1 - core, "etp": etp}

    def spot(arr, first, second):
        rel_x, rel_y = (second, first) if arr == 0 else (first, second)
        return lax.rem(col + rel_x, ring), lax.rem(etp + rel_y, etp_size)

    def block(arr, first, second):
        x_at, y_at = spot(arr, first, second)
        return rows.at[arr, x_at, y_at, core]

    sends = []

    def send(src, dst, recv_sem, device):
        slot = len(sends)
        copy = pltpu.make_async_remote_copy(src, dst, send_sem.at[slot], recv_sem, device_id=device, device_id_type=MESH)
        copy.start()
        sends.append(src.shape[0])

    def landed(ref, sem):
        pltpu.make_async_copy(ref, ref, sem).wait()

    def to_second(arr, first, src):
        dst = block(arr, first, 0)
        send(src, dst, near_sem.at[arr, first, 3], along_second[arr](1))
        send(src, dst, near_sem.at[arr, first, 1], along_second[arr](3))

    def to_peer(arr, first, second, src):
        send(src, block(arr, first, second), peer_sem.at[arr, first, second], partner)

    def first_own(arr):
        src = (u_ref, dy_ref)[arr]
        dst = block(arr, 0, 0)
        send(src, dst, near_sem.at[arr, 3, 0], along_first[arr](1))
        send(src, dst, near_sem.at[arr, 1, 0], along_first[arr](3))
        to_peer(arr, 0, 0, src)

    def second_own(arr):
        to_second(arr, 0, (u_ref, dy_ref)[arr])

    def event_first(arr, first):
        ref = block(arr, first, 0)
        landed(ref, near_sem.at[arr, first, 0])
        part = 0 if first == 3 else 1
        piece = ref.at[pl.ds(part * half, half)]
        send(piece, piece, half_sem.at[arr, part], along_first[arr](1 if first == 3 else 3))
        to_peer(arr, first, 0, ref)
        to_second(arr, first, ref)

    def event_far(arr):
        ref = block(arr, 2, 0)
        for part in PAIR:
            landed(ref.at[pl.ds(part * half, half)], half_sem.at[arr, part])
        to_peer(arr, 2, 0, ref)
        to_second(arr, 2, ref)

    def event_relay(arr, first):
        second = 3 if first in UP_SET else 1
        ref = block(arr, first, second)
        send(ref, ref, near_sem.at[arr, first, 2], along_second[arr](4 - second))

    def event_near(arr, first):
        for second in (3, 1):
            ref = block(arr, first, second)
            landed(ref, near_sem.at[arr, first, second])
            to_peer(arr, first, second, ref)

    def event_end(arr, first):
        ref = block(arr, first, 2)
        landed(ref, near_sem.at[arr, first, 2])
        to_peer(arr, first, 2, ref)

    def gate_copy(step):
        device, dest = other(step)
        return pltpu.make_async_remote_copy(gate_out.at[dest // etp_size], gate_in.at[lin], gate_send.at[step], gate_recv.at[lin], device_id=device, device_id_type=MESH)

    def start_gate(step, carry):
        gate_copy(step).start()
        return carry


    first_own(0)
    first_own(1)
    each_other(count, start_gate)
    gate_in[lin] = gate_out[ep]
    second_own(1)
    second_own(0)
    for arr, ref in enumerate((u_ref, dy_ref)):
        rows[arr, col, etp, core] = ref[...]

    lane_tile = 128
    for copy in w_copies:
        copy.wait()

    def flip(pos, carry):
        span = pl.ds(pl.multiple_of(pos * lane_tile, lane_tile), lane_tile)
        for src, dst in ((w1, wide.at[0]), (w3, wide.at[1]), (w2, wide.at[2])):
            dst[span, :] = src[:, span].T
        return carry

    lax.fori_loop(0, d_model // lane_tile, flip, 0)

    def wait_gate(step, carry):
        src = lax.rem(lin + step, count)
        landed(gate_in.at[src], gate_recv.at[src])
        return carry

    for first in (3, 1):
        for arr in PAIR:
            event_first(arr, first)

    def peer_wait(arr, site):
        first, second = (site[1], site[0]) if arr == 0 else (site[0], site[1])
        x_at, y_at = spot(arr, first, second)
        landed(rows.at[arr, x_at, y_at, 1 - core], peer_sem.at[arr, first, second])

    def event_gate():
        each_other(count, wait_gate)

    def both(event, *args):
        return [(event, (arr,) + args) for arr in PAIR]

    spots = ((col, etp), (etp, col))
    back_sends = []
    back_slot = {}

    def back(key, src, dst, device):
        slot = back_slot.setdefault(key, len(back_slot))
        copy = pltpu.make_async_remote_copy(src, dst, back_send.at[slot], back_recv.at[slot], device_id=device, device_id_type=MESH)
        copy.start()
        back_sends.append((slot, src.shape[0]))

    def arrive(key, ref):
        landed(ref, back_recv.at[back_slot[key]])

    def cell(ref, arr, first, sub):
        return ref.at[arr, lax.rem(spots[arr][0] + first, ring), lax.rem(spots[arr][1] + sub, ring)]

    def value(arr, first, sub):
        landed(cell(peer, arr, first, sub), swap_sem.at[arr, first, sub])
        return cell(mine, arr, first, sub)[...].astype(f32) + cell(peer, arr, first, sub)[...].astype(f32)

    def put(arr, first, sub, val):
        ref = cell(mine, arr, first, sub)
        ref[...] = val.astype(bf16)
        return ref

    far_slot = {2: 0, 1: 1, 3: 2, 0: 3}

    def back_far(arr, sub):
        device = along_stage(arr, sub in (2, 1))
        back(("far", arr, sub), put(arr, 2, sub, value(arr, 2, sub)), relay.at[arr, far_slot[sub]], device)

    def along_stage(arr, right):
        return along_second[arr](1 if right else 3)

    def back_direct(arr, sub):
        right = sub in (3, 0)
        first = 1 if right else 3
        back(("left" if right else "right", arr, sub), put(arr, first, sub, value(arr, first, sub)), inbox.at[arr, 0 if right else 1, sub], along_stage(arr, right))

    def back_relay(arr, sub):
        right = sub in (2, 1)
        first = 1 if right else 3
        incoming = relay.at[arr, far_slot[sub]]
        arrive(("far", arr, sub), incoming)
        val = value(arr, first, sub) + incoming[...].astype(f32)
        back(("left" if right else "right", arr, sub), put(arr, first, sub, val), inbox.at[arr, 0 if right else 1, sub], along_stage(arr, right))

    plan = {
        (0, 1): [(event_gate, ())] + both(event_near, 0),
        (0, 2): both(event_far) + both(event_relay, 0),
        (1, 2): both(event_near, 3) + both(event_relay, 3),
        (2, 1): both(event_near, 1) + both(event_relay, 1),
        (3, 1): both(event_near, 2) + both(event_relay, 2),
        (4, 0): both(back_direct, 0),
        (4, 1): both(event_end, 0),
        (4, 2): both(event_end, 3) + both(back_direct, 3),
        (4, 3): both(back_direct, 1),
        (5, 1): both(event_end, 1) + both(event_end, 2),
        (5, 2): [(back_far, (1, 0))],
        (6, 1): both(back_far, 0)[:1] + [(back_far, (0, 3)), (back_direct, (1, 2))],
        (7, 1): both(back_far, 1),
    }

    def run_events(unit, point):
        for pos in range(len(SITES)):
            todo = list(plan.get((pos, point), []))
            if point < 2:
                todo += [(peer_wait, (point, site)) for site in SITES[pos]]
            if todo:
                @pl.when(unit == pos)
                def _():
                    for event, args in todo:
                        event(*args)

    def act_copies(sites):
        copies = []
        for pos, (x_at, y_at) in enumerate(sites):
            site = (x_at * etp_size + y_at) * 2 * tok
            for kind in range(3):
                copies.append(pltpu.make_async_copy(act_buf.at[kind, pl.ds(pos * 2 * tok, 2 * tok)], act_hbm.at[kind, pl.ds(pl.multiple_of(site, 2 * tok), 2 * tok)], act_sem.at[pos, kind]))
        return copies

    def swap_copies(slot, sites, rels):
        copies = []
        for pos, (x_at, y_at) in enumerate(sites):
            rel_x, rel_y = rels[pos]
            away = 2 * pos + 1 - core
            copies.append(pltpu.make_async_remote_copy(y_buf.at[slot, away], peer.at[0, x_at, y_at], swap_send.at[slot, pos, 0], swap_sem.at[0, rel_x, rel_y], device_id=partner, device_id_type=MESH))
            copies.append(pltpu.make_async_remote_copy(du_buf.at[slot, away], peer.at[1, y_at, x_at], swap_send.at[slot, pos, 1], swap_sem.at[1, rel_y, rel_x], device_id=partner, device_id_type=MESH))
        return copies

    def wait_swaps(slot):
        for pos in PAIR:
            landed(y_buf.at[0, 0], swap_send.at[slot, pos, 0])
            landed(du_buf.at[0, 0], swap_send.at[slot, pos, 1])

    def sites_of(unit):
        out = []
        rels = []
        for pos in PAIR:
            rel_x = pick(unit, [entry[pos][0] for entry in SITES])
            rel_y = pick(unit, [entry[pos][1] for entry in SITES])
            out.append((lax.rem(col + rel_x, ring), lax.rem(etp + rel_y, etp_size)))
            rels.append((rel_x, rel_y))
        return out, rels

    def load(arr, sites):
        return jnp.concatenate([rows[arr, x_at, y_at].reshape(2 * tok, d_model) for x_at, y_at in sites], axis=0)

    def mm(lhs, rhs):
        return jnp.dot(lhs, rhs, preferred_element_type=f32)

    def unit_step(unit, carry):
        slot = lax.rem(unit, 2)
        sites, rels = sites_of(unit)
        run_events(unit, 0)

        @pl.when(unit >= 2)
        def _():
            wait_swaps(slot)

        x_rows = load(0, sites)
        h_buf[0] = mm(x_rows, wide[0, :d_model]).astype(bf16)
        h_buf[1] = mm(x_rows, wide[1, :d_model]).astype(bf16)
        run_events(unit, 1)
        @pl.when(unit >= 1)
        def _():
            for copy in act_copies(sites):
                copy.wait()

        q = mm(load(1, sites), wide[2, :d_model])
        cols = []
        lins = []
        for x_at, y_at in sites:
            for side in PAIR:
                src = (x_at * 2 + side) * etp_size + y_at
                lins.append(src)
                cols.append(gate_in[src].T[:tok])
        gate_cols = jnp.concatenate(cols, axis=0)
        lane = lax.broadcasted_iota(jnp.int32, q.shape, 1)
        spread = jnp.broadcast_to(gate_cols[:, local_exp - 1:local_exp], q.shape)
        for pos in range(local_exp - 2, -1, -1):
            spread = jnp.where(lane < (pos + 1) * width, gate_cols[:, pos:pos + 1], spread)
        live = spread > 0
        h1 = jnp.where(live, h_buf[0].astype(f32), 0.0)
        h3 = jnp.where(live, h_buf[1].astype(f32), 0.0)
        sig = jax.nn.sigmoid(h1)
        silu = h1 * sig
        act = (silu * h3).astype(bf16).astype(f32)
        ga = (spread * act).astype(bf16)
        act_buf[2] = ga
        y_buf[slot] = mm(ga, w2[...]).astype(bf16).reshape(4, tok, d_model)
        q = jnp.where(live, q, 0.0)
        da = (spread * q).astype(bf16).astype(f32)
        act_buf[0] = (da * h3 * (sig + silu * (1.0 - sig))).astype(bf16)
        act_buf[1] = (da * silu).astype(bf16)
        prod = act * q
        dg_wide = jnp.zeros((prod.shape[0], lane_tile), f32)
        lane_s = lax.broadcasted_iota(jnp.int32, dg_wide.shape, 1)
        for pos in range(local_exp):
            part_sum = jnp.zeros_like(dg_wide)
            for tile in range(pos * width // lane_tile, -(-(pos + 1) * width // lane_tile)):
                piece = prod[:, tile * lane_tile:(tile + 1) * lane_tile]
                low, high = pos * width - tile * lane_tile, (pos + 1) * width - tile * lane_tile
                if low > 0:
                    piece = jnp.where(lane_s >= low, piece, 0.0)
                if high < lane_tile:
                    piece = jnp.where(lane_s < high, piece, 0.0)
                part_sum = part_sum + piece
            dg_wide = jnp.where(lane_s == pos, jnp.sum(part_sum, axis=1, keepdims=True), dg_wide)
        for pos, src in enumerate(lins):
            dg_out[src] = jnp.concatenate([dg_wide[pos * tok:(pos + 1) * tok].T[:8], jnp.zeros((8, lane_tile - tok), f32)], axis=1)
        run_events(unit, 2)
        run_events(unit, 3)
        dx = mm(act_buf[0], w1[...]) + mm(act_buf[1], w3[...])
        du_buf[slot] = dx.astype(bf16).reshape(4, tok, d_model)
        for copy in act_copies(sites) + swap_copies(slot, sites, rels):
            copy.start()
        for pos, (x_at, y_at) in enumerate(sites):
            mine[0, x_at, y_at] = y_buf[slot, 2 * pos + core]
            mine[1, y_at, x_at] = du_buf[slot, 2 * pos + core]
        return carry

    lax.fori_loop(0, len(SITES), unit_step, 0)

    def dg_copy(step):
        device, dest = other(step)
        return pltpu.make_async_remote_copy(dg_out.at[dest], dg_in.at[lin], dg_send.at[step], dg_recv.at[lin], device_id=device, device_id_type=MESH)

    def dl_copy(step):
        device, dest = other(step)
        return pltpu.make_async_remote_copy(dl_out, dl_in.at[lin], dl_send.at[step], dl_recv.at[lin], device_id=device, device_id_type=MESH)

    def start_dg(step, carry):
        dg_copy(step).start()
        return carry

    each_other(count, start_dg)
    dg_in[lin] = dg_out[lin]
    for copy in act_copies(sites_of(0)[0]):
        copy.wait()
    act_loads = [pltpu.make_async_copy(act_hbm.at[kind], wide.at[kind], load_sem.at[kind]) for kind in range(3)]
    for copy in act_loads:
        copy.start()
    dw_outs = (dw1_hbm, dw3_hbm, dw2_hbm)
    inner = dw1_hbm.shape[0]
    chunk = dw_buf.shape[1]
    chunks = inner // chunk
    pending = {}
    todo = list(range(3 * chunks))

    def dw_steps(number):
        for _ in range(number):
            index = todo.pop(0)
            kind, part = divmod(index, chunks)
            if part == 0:
                act_loads[kind].wait()
            slot = index % 2
            if slot in pending:
                pending[slot].wait()
            lhs = wide[kind, :, part * chunk:(part + 1) * chunk]
            rhs = rows[kind // 2].reshape(count * tok, d_model)
            dw_buf[slot] = lax.dot_general(lhs, rhs, (((0,), (0,)), ((), ())), preferred_element_type=f32)
            pending[slot] = pltpu.make_async_copy(dw_buf.at[slot], dw_outs[kind].at[pl.ds(part * chunk, chunk)], dw_sem.at[slot])
            pending[slot].start()

    back_far(0, 2)
    back_far(1, 2)
    back_far(1, 3)
    back_direct(0, 2)
    for arr, sub in ((0, 0), (1, 0), (0, 3)):
        back_relay(arr, sub)
    dw_steps(2)
    for arr in PAIR:
        back_relay(arr, 1)

    def wait_dg(step, carry):
        src = lax.rem(lin + step, count)
        landed(dg_in.at[src], dg_recv.at[src])
        return carry

    each_other(count, wait_dg)
    tiles = []
    for group in range(2 * ring):
        tile = dg_in[group * etp_size]
        for part in range(1, etp_size):
            tile = tile + dg_in[group * etp_size + part]
        tiles.append(tile[:local_exp])
    d_gate = jnp.concatenate(tiles, axis=0)
    prob_all = prob_ref[...]
    d_logit = prob_all * (d_gate - jnp.sum(prob_all * d_gate, axis=0, keepdims=True))
    dl_out[...] = d_logit.astype(bf16)
    dl_in[lin] = d_logit.astype(bf16)

    def start_dl(step, carry):
        dl_copy(step).start()
        return carry

    each_other(count, start_dl)
    dw_steps(4)
    for arr, sub in ((0, 2), (1, 2), (1, 3)):
        back_relay(arr, sub)
    dw_steps(4)

    def settle(arr, sub):
        arrive(("left", arr, sub), inbox.at[arr, 0, sub])
        arrive(("right", arr, sub), inbox.at[arr, 1, sub])
        return value(arr, 0, sub) + inbox[arr, 0, sub].astype(f32) + inbox[arr, 1, sub].astype(f32)

    def ship(key, arr, sub, part, val, dst, step):
        rows_at = pl.ds(part * half, half)
        stage[arr, sub - 1, rows_at] = val.astype(bf16)
        back(key, stage.at[arr, sub - 1, rows_at], dst, along_first[arr](step))

    for arr in PAIR:
        val = settle(arr, 1)
        ship(("left2", arr, 1), arr, 1, 1, val[half:], inbox2.at[arr, 0, 1], 1)
        total[arr, 0, :half] = val[:half]
    for arr in PAIR:
        val = settle(arr, 2)
        ship(("far2", arr, 0), arr, 2, 0, val[:half], relay2.at[arr, 0], 1)
        ship(("far2", arr, 1), arr, 2, 1, val[half:], relay2.at[arr, 1], 3)
    for arr in PAIR:
        val = settle(arr, 3)
        ship(("right2", arr, 0), arr, 3, 0, val[:half], inbox2.at[arr, 1, 0], 3)
        total[arr, 0, half:] = val[half:]
    dw_steps(2)
    for arr in PAIR:
        arrive(("far2", arr, 0), relay2.at[arr, 0])
        val = total[arr, 0, :half] + relay2[arr, 0].astype(f32)
        ship(("left2", arr, 0), arr, 1, 0, val, inbox2.at[arr, 0, 0], 1)
        arrive(("far2", arr, 1), relay2.at[arr, 1])
        val = total[arr, 0, half:] + relay2[arr, 1].astype(f32)
        ship(("right2", arr, 1), arr, 3, 1, val, inbox2.at[arr, 1, 1], 3)
    for arr in PAIR:
        total[arr, 1] = settle(arr, 0)

    def wait_dl(step, carry):
        src = lax.rem(lin + step, count)
        landed(dl_in.at[src], dl_recv.at[src])
        return carry

    each_other(count, wait_dl)
    du_router = lax.dot_general(dl_out[...], wr_ref[...], (((0,), (0,)), ((), ())), preferred_element_type=f32)[:tok]
    dwr_out[...] = jnp.zeros_like(dwr_out)

    def dwr_step(idx, carry):
        parts = []
        for pair in range(etp_size):
            low = dl_in[idx * 2 * etp_size + pair].astype(f32)
            high = dl_in[(idx * 2 + 1) * etp_size + pair].astype(f32)
            parts.append((low + pltpu.roll(high, tok, 1)).astype(bf16))
        dwr_out[...] += mm(jnp.concatenate(parts, axis=1), rows[0, idx].reshape(2 * etp_size * tok, d_model))
        return carry

    lax.fori_loop(0, ring, dwr_step, 0)
    dw_steps(len(todo))
    for part in PAIR:
        for arr, base, out in ((0, u_ref, y_out), (1, dy_ref, du_out)):
            arrive(("left2", arr, part), inbox2.at[arr, 0, part])
            arrive(("right2", arr, part), inbox2.at[arr, 1, part])
            rows_at = pl.ds(part * half, half)
            val = base[rows_at].astype(f32) + total[arr, 1, rows_at] + inbox2[arr, 0, part].astype(f32) + inbox2[arr, 1, part].astype(f32)
            if arr == 1:
                val = val + du_router[part * half:(part + 1) * half]
            out[rows_at] = val.astype(bf16)
    for slot in PAIR:
        wait_swaps(slot)
    for copy in pending.values():
        copy.wait()
    for slot, size in enumerate(sends):
        landed(rows.at[0, 0, 0, 0, pl.ds(0, size)], send_sem.at[slot])
    for slot, size in back_sends:
        landed(rows.at[0, 0, 0, 0, pl.ds(0, size)], back_send.at[slot])

    def drain(step, carry):
        gate_copy(step).wait_send()
        dg_copy(step).wait_send()
        dl_copy(step).wait_send()
        return carry

    each_other(count, drain)


def block_call(mesh, u_loc, dy_loc, ids_t, wr_t, w1, w3, w2):
    etp_size, ep_size = mesh.shape["etp"], mesh.shape["ep"]
    tok, d_model = u_loc.shape
    experts, inner = wr_t.shape[0], w1.shape[0]
    count, ring, half = etp_size * ep_size, ep_size // 2, tok // 2
    assert ring == 4 and etp_size == 4
    width = inner // (experts // ep_size)
    vmem = pl.BlockSpec(memory_space=pltpu.VMEM)
    hbm = pl.BlockSpec(memory_space=pl.ANY)
    bf16, f32 = jnp.bfloat16, jnp.float32
    dma = pltpu.SemaphoreType.DMA
    shape = jax.ShapeDtypeStruct
    quad = (2, ring, etp_size)
    return pl.pallas_call(
        functools.partial(block_kernel, etp_size, ring, width),
        out_shape=(shape((tok, d_model), bf16),) * 2 + (shape((experts, d_model), f32),) + (shape((inner, d_model), f32),) * 3 + (shape((3, count * tok, inner), bf16),),
        in_specs=[vmem] * 4 + [hbm] * 3,
        out_specs=(vmem,) * 3 + (hbm,) * 4,
        scratch_shapes=[
            pltpu.VMEM(quad + (2, tok, d_model), bf16),
            pltpu.VMEM((inner, d_model), bf16), pltpu.VMEM((inner, d_model), bf16), pltpu.VMEM((inner, d_model), bf16),
            pltpu.VMEM((3, count * tok, inner), bf16),
            pltpu.VMEM((2, 4, tok, d_model), bf16), pltpu.VMEM((2, 4, tok, d_model), bf16), pltpu.VMEM((3, 4 * tok, inner), bf16), pltpu.VMEM((2, 4 * tok, inner), bf16),
            pltpu.VMEM((ep_size, 8, 128), f32), pltpu.VMEM((count, 8, 128), f32), pltpu.VMEM((count, 8, 128), f32), pltpu.VMEM((experts, 128), f32),
            pltpu.VMEM(quad + (tok, d_model), bf16), pltpu.VMEM(quad + (tok, d_model), bf16),
            pltpu.VMEM((2, 4, tok, d_model), bf16),
            pltpu.VMEM((2, 2, 4, tok, d_model), bf16),
            pltpu.VMEM((2, 2, tok, d_model), f32),
            pltpu.VMEM((2, 3, tok, d_model), bf16),
            pltpu.VMEM((2, 2, half, d_model), bf16),
            pltpu.VMEM((2, 2, 2, half, d_model), bf16),
            pltpu.VMEM((2, 128, d_model), f32),
            pltpu.VMEM((count, 8, 128), f32),
            pltpu.VMEM((count, experts, 128), bf16),
            pltpu.VMEM((experts, 128), bf16),
            dma((3,)), dma((2, 3)), dma((72,)), dma(quad), dma((2, 2)), dma(quad), dma((count,)), dma((count,)),
            dma((2, 2, 2)), dma(quad), dma((48,)), dma((48,)), dma((3,)), dma((2,)), dma((count,)), dma((count,)), dma((count,)), dma((count,)),
        ],
        compiler_params=pltpu.CompilerParams(collective_id=0, has_side_effects=True, vmem_limit_bytes=67043328),
        name="moe_block",
    )(u_loc, dy_loc, ids_t, wr_t, w1, w3, w2)[:6]


def copy_kernel(number, *refs):
    srcs, dsts, bufs = refs[:number], refs[number:2 * number], refs[2 * number:3 * number]
    in_sem, out_sem = refs[3 * number:]
    loads, stores = [], []
    for src, dst, buf in zip(srcs, dsts, bufs):
        step = min(src.shape[0], 256)
        for start in range(0, src.shape[0], step):
            at = pl.ds(start, step)
            loads.append(pltpu.make_async_copy(src.at[at], buf.at[at], in_sem.at[len(loads)]))
            stores.append(pltpu.make_async_copy(buf.at[at], dst.at[at], out_sem.at[len(stores)]))
    for copy in loads:
        copy.start()
    for load, store in zip(loads, stores):
        load.wait()
        store.start()
    for copy in stores:
        copy.wait()


def copy_call(arrays):
    hbm = pl.BlockSpec(memory_space=pltpu.HBM)
    return pl.pallas_call(
        functools.partial(copy_kernel, len(arrays)),
        out_shape=tuple(jax.ShapeDtypeStruct(a.shape, a.dtype) for a in arrays),
        in_specs=[hbm] * len(arrays),
        out_specs=(hbm,) * len(arrays),
        scratch_shapes=[pltpu.VMEM(a.shape, a.dtype) for a in arrays] + [pltpu.SemaphoreType.DMA((16,)), pltpu.SemaphoreType.DMA((16,))],
        compiler_params=pltpu.CompilerParams(vmem_limit_bytes=67043328),
        name="place_results",
    )(*arrays)


def solution(mesh):
    tok_spec = P(("dp", "ep", "etp"), None)
    col_spec = P("ep", None, "etp")
    row_spec = P("ep", "etp", None)
    in_specs = (tok_spec, tok_spec, tok_spec, P(None, None), col_spec, col_spec, row_spec)
    out_specs = (tok_spec, tok_spec, P(("dp", "ep"), None, "etp"), P(("dp", "ep"), None, "etp"), P(("dp", "ep"), "etp", None), P("dp", None))

    def device_step(u_loc, dy_loc, ids_loc, w_router, w_gate, w_up, w_down):
        local_exp, d_model, width = w_gate.shape
        inner = local_exp * width
        w1 = jnp.swapaxes(w_gate, 1, 2).reshape(inner, d_model)
        w3 = jnp.swapaxes(w_up, 1, 2).reshape(inner, d_model)
        w2 = w_down.reshape(inner, d_model)
        y_loc, du_loc, dwr_t, dw1, dw3, dw2 = copy_call(block_call(mesh, u_loc, dy_loc, ids_loc.T, w_router.T, w1, w3, w2))
        unfold = lambda d: jnp.swapaxes(d.reshape(local_exp, width, d_model), 1, 2)
        return y_loc, du_loc, unfold(dw1), unfold(dw3), dw2.reshape(local_exp, width, d_model), dwr_t.T

    return jax.shard_map(device_step, mesh=mesh, in_specs=in_specs, out_specs=out_specs, check_vma=False)
```
